256 devices in a mesh: groups: 2 (over y), ctx: 128 (over z, x, core).
Axes of the slice: x: 4, y: 2, z: 16, core: 2. Of those that a mesh axis runs over, the one named last changes fastest.
The devices are a block of a 4x16x16 slice.
Arguments:
- queries: bfloat16 [512, 5120], P('groups'), parts along dimension 0, may hold values from -400 to 400
- new_keys: bfloat16 [512, 5120], P(('groups', 'ctx')), parts along dimension 0, may hold values from -15 to 15
- new_values: bfloat16 [512, 5120], P(('groups', 'ctx')), parts along dimension 0, may hold values from -6 to 6
- cache_keys: bfloat16 [8, 256, 32, 5120], P('groups', 'ctx'), parts along dimension 0, may hold values from -5 to 5
- cache_values: bfloat16 [8, 256, 32, 5120], P('groups', 'ctx'), parts along dimension 0, may hold values from -6 to 6
- slot_of: int32 [8], P('groups'), parts along dimension 0, may hold values from 0 to 3, as said below
- cached: int32 [8], P('groups'), parts along dimension 0, may hold values from 1 to 256, as said below
- actions: int32 [8, 8], P('groups'), parts along dimension 0, may hold values from 0 to 255
- action_table: bfloat16 [256, 5120], replicated, may hold values from -3 to 3
- null_gate: float32 [5120], replicated, may hold values from -3 to 3
- residual: bfloat16 [512, 5120], P(('groups', 'ctx')), parts along dimension 0, may hold values from -3 to 3
- out_weight: bfloat16 [5120, 5120], P('ctx'), may hold values from -0.078125 to 0.078125
Outputs:
- branch_out: bfloat16 [512, 5120], P(('groups', 'ctx')), parts along dimension 0
The draws below stay inside these ranges and needn't reach their ends.
There are 2 independent parts, one for each index of `groups`. The reference program is written for one: setup_inputs(seed, part) draws one part's arguments, and reference() takes and returns one part's arrays. A program takes and returns all parts, laid end to end along the dimension named above; an argument that names none is the same for every part. Nothing has to cross between parts.
Inputs may be any that keep to these rules, and one draw needn't show every extreme that they name: `slot_of`: the 4 sessions have different slots. Some session has all 256 frames cached.
All inputs are finite; a program needn't handle non-finite values.
Results may differ from the reference program's by a relative error of at most 0.0042.
Values may be sent and summed in bfloat16 or wider, within the bound.
A program may use at most 128 MiB of HBM per device.

```python
import math
import jax
import jax.numpy as jnp
from jax import lax

D = 5120
HEADS = 40
SESS = 4
NEWTOK = 32
ACTS = 8
VOCAB = 256
FRAMES = 256
ROWS = 256


def shared_layout(key):
    base_key = jax.random.fold_in(key, 7)
    slot_order = jax.random.permutation(jax.random.fold_in(base_key, 1), SESS).astype(jnp.int32)
    lengths = jax.random.randint(jax.random.fold_in(base_key, 2), (SESS,), 1, FRAMES + 1)
    longest = jax.random.randint(jax.random.fold_in(base_key, 3), (), 0, SESS)
    lengths = jnp.where(jnp.arange(SESS) == longest, FRAMES, lengths).astype(jnp.int32)
    shape = (SESS, 2 * NEWTOK, HEADS)
    frame_pick = jax.random.randint(jax.random.fold_in(base_key, 4), shape, 0, lengths[:, None, None])
    token_pick = jax.random.randint(jax.random.fold_in(base_key, 5), shape, 0, NEWTOK)
    return (slot_order, lengths, frame_pick, token_pick)


def base_keys(key):
    raw = jax.random.normal(jax.random.fold_in(key, 76), (SESS, FRAMES, NEWTOK, HEADS, D // HEADS), jnp.float32)
    return jnp.clip(raw, -5.0, 5.0)


def drawn_keys(keys, slot_order, frame_pick, token_pick):
    head_ids = jnp.arange(HEADS)[None, None, :]
    return keys[slot_order[:, None, None], frame_pick, token_pick, head_ids]


def draw_slot_of(key, part):
    return shared_layout(key)[0]


def draw_cached(key, part):
    return shared_layout(key)[1]


def draw_new_keys(key, part):
    spread = 2.5
    raw = jax.random.normal(jax.random.fold_in(key, 91), (2 * SESS * NEWTOK, D), jnp.float32) * spread
    return jnp.clip(raw, -15.0, 15.0).astype(jnp.bfloat16)


def draw_cache_keys(key, part):
    keys = base_keys(key)
    return keys.reshape(SESS, FRAMES, NEWTOK, D).astype(jnp.bfloat16)


def draw_queries(key, part):
    slot_order, lengths, frame_pick, token_pick = shared_layout(key)
    keys = base_keys(key)
    aligned = drawn_keys(keys, slot_order, frame_pick, token_pick)
    noise = jax.random.normal(jax.random.fold_in(key, 83), aligned.shape, jnp.float32)
    result = 0.88 * aligned + noise
    result = jnp.clip(result, -400.0, 400.0)
    return result.reshape(SESS * 2 * NEWTOK, D).astype(jnp.bfloat16)


def with_ends(values, own_key, smallest, high):
    longest = values.shape.index(max(values.shape))
    spots = []
    for shift in (0, 1):
        where = [jax.random.randint(jax.random.fold_in(own_key, axis), (), 0, length) for axis, length in enumerate(values.shape)]
        where[longest] = (where[longest] + shift) % values.shape[longest]
        spots.append(tuple(where))
    return values.at[spots[0]].set(smallest).at[spots[1]].set(high)


def steps_of(stream_key, dims, shards, low, top_value):
    loudness, own = 1.0, jax.random.fold_in(stream_key, 6)
    for axis_at, blocks in shards:
        draws = jnp.exp(jax.random.uniform(jax.random.fold_in(own, axis_at), (blocks,), jnp.float32, low / len(shards), top_value / len(shards)))
        loudness = loudness * jnp.repeat(draws, dims[axis_at] // blocks).reshape([-1 if axis == axis_at else 1 for axis in range(len(dims))])
    return loudness


def scatter_about(key, extent, scale, limit, pieces=(), held_as=jnp.bfloat16):
    drawn = jax.random.normal(key, extent, jnp.float32) * scale
    if len(pieces) > 0:
        drawn = steps_of(key, extent, pieces, -0.22, 0.18) * drawn
    return jnp.clip(drawn, min=-limit, max=limit).astype(held_as)


def setup_inputs(seed: int = 0, part: int = 0) -> dict:
    splits = jax.random.split(jax.random.key(seed), 13)
    part_keys = jax.random.split(jax.random.fold_in(splits[12], part), 13)
    return {
        "queries": draw_queries(jax.random.fold_in(jax.random.fold_in(splits[12], part), 71), part),
        "new_keys": draw_new_keys(jax.random.fold_in(jax.random.fold_in(splits[12], part), 71), part),
        "new_values": scatter_about(part_keys[2], (ROWS, D), 1.0, 6.0, ((0, 128),)),
        "cache_keys": draw_cache_keys(jax.random.fold_in(jax.random.fold_in(splits[12], part), 71), part),
        "cache_values": scatter_about(part_keys[4], (SESS, FRAMES, NEWTOK, D), 1.0, 6.0, ((1, 128),)),
        "slot_of": draw_slot_of(jax.random.fold_in(jax.random.fold_in(splits[12], part), 71), part),
        "cached": draw_cached(jax.random.fold_in(jax.random.fold_in(splits[12], part), 71), part),
        "actions": with_ends(jax.random.randint(part_keys[7], (SESS, ACTS), 0, VOCAB), jax.random.fold_in(part_keys[7], 1), 0, VOCAB - 1).astype(jnp.int32),
        "action_table": scatter_about(splits[8], (VOCAB, D), 0.5, 3.0),
        "null_gate": scatter_about(splits[9], (D,), 0.5, 3.0, (), jnp.float32),
        "residual": scatter_about(part_keys[10], (ROWS, D), 0.5, 3.0, ((0, 128),)),
        "out_weight": scatter_about(splits[11], (D, D), D ** -0.5, 0.078125, ((0, 128),)),
    }


masked_score = -1e+30

def rounded(values):
    return lax.optimization_barrier(values.astype(jnp.bfloat16)).astype(jnp.float32)

def reference(queries, new_keys, new_values, cache_keys, cache_values, slot_of, cached, actions, action_table, null_gate, residual, out_weight):
    total_rows, model_dim = queries.shape
    head_dim = model_dim // HEADS
    scaling = 1.0 / math.sqrt(head_dim)
    session_rows = 2 * NEWTOK
    frame_keys = FRAMES * NEWTOK
    branch_ids = jnp.arange(session_rows) % 2
    own_mask = branch_ids[:, None] == branch_ids[None, :]
    frame_ids = jnp.arange(frame_keys) // NEWTOK
    blocks = []
    for session in range(SESS):
        row_start = session * session_rows
        block_queries = queries[row_start:row_start + session_rows].astype(jnp.float32).reshape(session_rows, HEADS, head_dim)
        slot_index = slot_of[session]
        slot_keys = lax.dynamic_index_in_dim(cache_keys, slot_index, 0, keepdims=False).astype(jnp.float32).reshape(frame_keys, HEADS, head_dim)
        slot_values = lax.dynamic_index_in_dim(cache_values, slot_index, 0, keepdims=False).astype(jnp.float32).reshape(frame_keys, HEADS, head_dim)
        own_keys = new_keys[row_start:row_start + session_rows].astype(jnp.float32).reshape(session_rows, HEADS, head_dim)
        own_values = new_values[row_start:row_start + session_rows].astype(jnp.float32).reshape(session_rows, HEADS, head_dim)
        cache_scores = jnp.einsum('qhd,khd->hqk', block_queries, slot_keys, precision=lax.Precision.HIGHEST) * scaling
        cache_scores = jnp.where((frame_ids < cached[session])[None, None, :], cache_scores, masked_score)
        own_scores = jnp.einsum('qhd,khd->hqk', block_queries, own_keys, precision=lax.Precision.HIGHEST) * scaling
        own_scores = jnp.where(own_mask[None], own_scores, masked_score)
        highest = jnp.maximum(cache_scores.max(-1), own_scores.max(-1))
        cache_weights = jnp.exp(cache_scores - highest[..., None])
        own_weights = jnp.exp(own_scores - highest[..., None])
        totals = cache_weights.sum(-1) + own_weights.sum(-1)
        numer = jnp.einsum('hqk,khd->qhd', rounded(cache_weights), slot_values, precision=lax.Precision.HIGHEST)
        numer = numer + jnp.einsum('hqk,khd->qhd', rounded(own_weights), own_values, precision=lax.Precision.HIGHEST)
        blocks.append((numer / totals.T[:, :, None]).astype(jnp.bfloat16).reshape(session_rows, model_dim))
    attended = jnp.concatenate(blocks, 0)
    vocab_size = action_table.shape[0]
    action_counts = (actions[:, :, None] == jnp.arange(vocab_size, dtype=jnp.int32)[None, None, :]).astype(jnp.float32).sum(1)
    cond_gate = 1.0 + jnp.dot(action_counts.astype(jnp.bfloat16), action_table, preferred_element_type=jnp.float32) / actions.shape[1]
    uncond_gate = 1.0 + null_gate
    projected = jnp.dot(attended, out_weight, preferred_element_type=jnp.float32)
    cond_rows = jnp.repeat(cond_gate, NEWTOK, axis=0)
    uncond_rows = jnp.broadcast_to(uncond_gate[None, :], cond_rows.shape)
    gate_rows = jnp.stack([cond_rows, uncond_rows], 1).reshape(total_rows, model_dim)
    return (residual.astype(jnp.float32) + gate_rows * projected).astype(jnp.bfloat16)
```

```python
import functools
import math

import jax
import jax.numpy as jnp
from jax import lax
from jax.experimental import pallas as pl
from jax.experimental.pallas import tpu as pltpu
from jax.sharding import Mesh
from jax.sharding import PartitionSpec as P

HEAD = 128
PIECE = 16
CTX = ("z", "x", "core")
GROUPS_CTX = ("groups", "z", "x", "core")
MESH = pl.DeviceIdType.MESH
MASKED = -1e30
F32 = jnp.float32
BF16 = jnp.bfloat16


def attend_kernel(
    per_step,
    places,
    slot_ref,
    cached_ref,
    act_ref,
    q_ref,
    k_ref,
    v_ref,
    nk_ref,
    nv_ref,
    table_ref,
    num_ref,
    ml_ref,
    gate_ref,
    bias_ref,
    count_ref,
):
    step = pl.program_id(0)
    slots, frames, tokens, _ = k_ref.shape
    sessions, acts = act_ref.shape
    rows = q_ref.shape[0]
    half = rows // 2
    session_rows = rows // sessions
    own = nk_ref.shape[0]
    keys = slots * frames * tokens
    _, nx, nc = places
    factor = math.log2(math.e) / math.sqrt(HEAD)

    @pl.when(step == 0)
    def _():
        pos = (lax.axis_index("z") * nx + lax.axis_index("x")) * nc + lax.axis_index("core")
        key = lax.broadcasted_iota(jnp.int32, (keys, rows), 0)
        row = lax.broadcasted_iota(jnp.int32, (keys, rows), 1)
        live = jnp.zeros((keys, rows), jnp.int32)
        for s in range(sessions):
            count = jnp.clip(cached_ref[s] - pos * frames, 0, frames) * tokens
            base = slot_ref[s] * (frames * tokens)
            here = (row >= s * session_rows) & (row < (s + 1) * session_rows)
            live = jnp.where(here & (key >= base) & (key < base + count), 1, live)
        bias_ref[0:keys, :] = jnp.where(live == 1, 0.0, MASKED)
        key = lax.broadcasted_iota(jnp.int32, (PIECE, rows), 0)
        row = lax.broadcasted_iota(jnp.int32, (PIECE, rows), 1)
        first = pos * own
        session = first // session_rows
        low = session * session_rows
        good = (row >= low) & (row < low + session_rows) & (key < own)
        good = good & (((row - first - key) & 1) == 0)
        bias_ref[keys : keys + PIECE, :] = jnp.where(good, 0.0, MASKED)
        vocab = table_ref.shape[0]
        lane = lax.broadcasted_iota(jnp.int32, (8, vocab), 1)
        sums = jnp.zeros((8, vocab), F32)
        for a in range(acts):
            sums = sums + jnp.where(lane == act_ref[session, a], 1.0, 0.0)
        count_ref[...] = sums

    spot = lax.broadcasted_iota(jnp.int32, (PIECE, HEAD), 0)

    def few(ref, cols):
        values = jnp.zeros((PIECE, HEAD), F32)
        for j in range(own):
            values = jnp.where(spot == j, ref[j : j + 1, cols].astype(F32), values)
        return values.astype(BF16)

    last = (((1,), (1,)), ((), ()))
    first_dims = (((0,), (0,)), ((), ()))
    for i in range(per_step):
        cols = slice(i * HEAD, (i + 1) * HEAD)
        q = q_ref[:, cols]
        k = k_ref[:, :, :, cols].reshape(keys, HEAD)
        v = v_ref[:, :, :, cols].reshape(keys, HEAD)
        s1 = lax.dot_general(k, q, last, preferred_element_type=F32)
        s2 = lax.dot_general(few(nk_ref, cols), q, last, preferred_element_type=F32)
        s1 = s1 * factor + bias_ref[0:keys, :]
        s2 = s2 * factor + bias_ref[keys : keys + PIECE, :]
        top = jnp.maximum(jnp.max(s1, 0, keepdims=True), jnp.max(s2, 0, keepdims=True))
        p1 = jnp.exp2(s1 - top)
        p2 = jnp.exp2(s2 - top)
        total = jnp.sum(p1, 0, keepdims=True) + jnp.sum(p2, 0, keepdims=True)
        numer = lax.dot_general(v, p1.astype(BF16), first_dims, preferred_element_type=F32)
        numer = numer + lax.dot_general(
            few(nv_ref, cols), p2.astype(BF16), first_dims, preferred_element_type=F32
        )
        numer = numer.astype(num_ref.dtype)
        head = step * per_step + i
        for c in range(2):
            part = slice(c * half, (c + 1) * half)
            num_ref[c, cols, :] = numer[:, part]
            ml_ref[c, 0, pl.ds(head, 1), :] = top[:, part]
            ml_ref[c, 1, pl.ds(head, 1), :] = total[:, part]
    sums = jnp.dot(count_ref[...].astype(BF16), table_ref[...], preferred_element_type=F32)
    gate_ref[...] = 1.0 + sums[0:1, :] / acts


def attend(queries, nk, nv, keys, values, slot_of, cached, actions, table, places):
    rows, model_dim = queries.shape
    heads = model_dim // HEAD
    per_step = 4 if heads % 4 == 0 else 1
    width = per_step * HEAD
    slots, frames, tokens, _ = keys.shape
    own = nk.shape[0]
    vocab = table.shape[0]
    flat = lambda n: pl.BlockSpec((n, width), lambda i, *_: (0, i))
    block = pl.BlockSpec((slots, frames, tokens, width), lambda i, *_: (0, 0, 0, i))
    half = rows // 2
    return pl.pallas_call(
        functools.partial(attend_kernel, per_step, places),
        grid_spec=pltpu.PrefetchScalarGridSpec(
            num_scalar_prefetch=3,
            grid=(heads // per_step,),
            in_specs=[flat(rows), block, block, flat(own), flat(own), flat(vocab)],
            out_specs=[
                pl.BlockSpec((2, width, half), lambda i, *_: (0, i, 0)),
                pl.BlockSpec((2, 2, heads, half), lambda i, *_: (0, 0, 0, 0)),
                flat(1),
            ],
            scratch_shapes=[
                pltpu.VMEM((slots * frames * tokens + PIECE, rows), F32),
                pltpu.VMEM((8, vocab), F32),
            ],
        ),
        out_shape=[
            jax.ShapeDtypeStruct((2, model_dim, half), BF16),
            jax.ShapeDtypeStruct((2, 2, heads, half), F32),
            jax.ShapeDtypeStruct((1, model_dim), F32),
        ],
        compiler_params=pltpu.CompilerParams(dimension_semantics=("arbitrary",)),
        name="attend",
    )(slot_of, cached, actions, queries, keys, values, nk, nv, table)


def join_kernel(places, lag, num_ref, ml_ref, w_ref, gate_ref, null_ref, res_ref, out_ref, *rest):
    (
        mlr, scale, joint, ra, d, rel, relout, fin1, fin2, xs, zr, zms, zmr, fz, acc,
        attg, wbuf, pr, prr, fin, finr,
        ml_s, ml_r, a_s, a_r, o_s, o_r, d_s, d_r, r_s, r_r, z_s, z_r, zm_s, zm_r,
        at_s, at_r, w_s, w_r, p_s, p_r, f_s, f_r,
    ) = rest
    nz, nx, nc = places
    near = nx * nc
    z, x, c = (lax.axis_index(name) for name in CTX)
    me = x * nc + c
    heads = ml_ref.shape[2]
    model_dim = num_ref.shape[1]
    wide = model_dim // nz
    blk = wide // nx
    pieces = blk // PIECE
    per_head = HEAD // PIECE
    cols = model_dim // near
    wrows = w_ref.shape[0]

    def near_id(j):
        return {"x": j // nc, "core": lax.rem(j, nc)}

    def send(src, dst, ssem, rsem, where):
        copy = pltpu.make_async_remote_copy(
            src_ref=src, dst_ref=dst, send_sem=ssem, recv_sem=rsem,
            device_id=where, device_id_type=MESH,
        )
        copy.start()

    def got(dst, sem):
        pltpu.make_async_remote_copy(
            src_ref=dst, dst_ref=dst, send_sem=sem, recv_sem=sem,
            device_id={"core": 1 - c}, device_id_type=MESH,
        ).wait_recv()

    def gone(src, sem):
        pltpu.make_async_remote_copy(
            src_ref=src, dst_ref=src, send_sem=sem, recv_sem=sem,
            device_id={"core": 1 - c}, device_id_type=MESH,
        ).wait_send()

    def near_peer(i):
        return lax.rem(me + i, near)

    def far_peer(i):
        return lax.rem(z + i, nz)

    barrier = pltpu.get_barrier_semaphore()

    @pl.loop(1, near)
    def _(i):
        pl.semaphore_signal(barrier, inc=1, device_id=near_id(near_peer(i)), device_id_type=MESH)

    @pl.loop(1, nz)
    def _(i):
        pl.semaphore_signal(barrier, inc=1, device_id={"z": far_peer(i)}, device_id_type=MESH)

    pl.semaphore_wait(barrier, near + nz - 2)

    def turn(k):
        odd = lax.rem(k, 2)
        ahead = nz // 2 + odd * ((k + 1) // 2) - (1 - odd) * (k // 2)
        return lax.rem(z + ahead, nz)

    @pl.loop(1, near)
    def _(i):
        j = near_peer(i)
        send(ml_ref.at[lax.rem(j, nc)], mlr.at[me], ml_s.at[j], ml_r.at[me], near_id(j))

    @pl.loop(0, nz)
    def _(k):
        t = turn(k)
        part = pl.ds(pl.multiple_of(t * wide, PIECE), wide)
        send(num_ref.at[1 - c, part], ra.at[part], a_s.at[t], a_r.at[t], {"core": 1 - c})

    mlr[me] = ml_ref[c]

    @pl.loop(1, near)
    def _(i):
        j = near_peer(i)
        got(mlr.at[j], ml_r.at[j])

    top = mlr[0, 0]
    for j in range(1, near):
        top = jnp.maximum(top, mlr[j, 0])
    total = jnp.zeros_like(top)
    for j in range(near):
        total = total + mlr[j, 1] * jnp.exp2(mlr[j, 0] - top)
    scale[0] = jnp.exp2(ml_ref[c, 0] - top)
    scale[1] = jnp.exp2(mlr[x * nc + 1 - c, 0] - top)
    joint[0] = top
    joint[1] = total

    @pl.loop(0, nz)
    def _(t):
        low = (t * (wide // PIECE) + x * pieces) // per_head
        high = jnp.minimum(low + 1, heads - 1)
        zms[t, 0:1, :] = joint[0, pl.ds(low, 1), :]
        zms[t, 1:2, :] = joint[0, pl.ds(high, 1), :]
        zms[t, 2:3, :] = joint[1, pl.ds(low, 1), :]
        zms[t, 3:4, :] = joint[1, pl.ds(high, 1), :]
        zms[t, 4:8, :] = jnp.zeros((4, zms.shape[2]), F32)

    @pl.loop(1, nz)
    def _(i):
        t = far_peer(i)
        send(zms.at[t], zmr.at[z], zm_s.at[t], zm_r.at[z], {"z": t})

    def ways(t):
        back = lax.rem(t, 2)
        ahead = lax.rem(x + 1 + (nx - 2) * back, nx)
        behind = lax.rem(x + nx - 1 - (nx - 2) * back, nx)
        return ahead, behind

    opposite = lax.rem(x + nx // 2, nx)

    def rows_of(t, xx):
        return pl.ds(pl.multiple_of(t * wide + xx * blk, PIECE), blk)

    def merge(k):
        t = turn(k)
        part = pl.ds(pl.multiple_of(t * wide, PIECE), wide)
        got(ra.at[part], a_r.at[t])
        for i in range(wide // PIECE):
            g = t * (wide // PIECE) + i
            h = g // per_head
            r = pl.ds(pl.multiple_of(g * PIECE, PIECE), PIECE)
            mine = num_ref[c, r, :].astype(F32) * scale[0, pl.ds(h, 1), :]
            other = ra[r, :].astype(F32) * scale[1, pl.ds(h, 1), :]
            d[r, :] = (mine + other).astype(BF16)
        ahead, behind = ways(t)
        send(d.at[rows_of(t, opposite)], rel.at[t], o_s.at[t], o_r.at[t], {"x": ahead})
        send(d.at[rows_of(t, behind)], fin2.at[t], d_s.at[t], d_r.at[t], {"x": behind})

    def relay(k):
        t = turn(k)
        ahead, _ = ways(t)
        got(rel.at[t], o_r.at[t])
        relout[t] = (rel[t].astype(F32) + d[rows_of(t, ahead), :].astype(F32)).astype(BF16)
        send(relout.at[t], fin1.at[t], r_s.at[t], r_r.at[t], {"x": ahead})

    def settle(k):
        t = turn(k)
        got(fin1.at[t], r_r.at[t])
        got(fin2.at[t], d_r.at[t])
        sums = fin1[t].astype(F32) + fin2[t].astype(F32) + d[rows_of(t, x), :].astype(F32)
        xs[t] = sums.astype(BF16)

        @pl.when(k < nz - 1)
        def _():
            send(xs.at[t], zr.at[z], z_s.at[t], z_r.at[z], {"z": t})

    @pl.loop(0, nz + 2 * lag)
    def _(k):
        @pl.when(k < nz)
        def _():
            merge(k)

        @pl.when((k >= lag) & (k < nz + lag))
        def _():
            relay(k - lag)

        @pl.when(k >= 2 * lag)
        def _():
            settle(k - 2 * lag)

    def wpart(j):
        return pl.ds(pl.multiple_of(j * cols, cols), cols)

    @pl.loop(1, near)
    def _(i):
        j = near_peer(i)
        send(w_ref.at[:, wpart(j)], wbuf.at[me], w_s.at[j], w_r.at[me], near_id(j))

    wbuf[me] = w_ref[:, wpart(me)]
    zr[z] = xs[z]
    zmr[z] = zms[z]

    @pl.loop(1, nz)
    def _(i):
        t = far_peer(i)
        got(zmr.at[t], zm_r.at[t])

    top = zmr[0, 0:2, :]
    for t in range(1, nz):
        top = jnp.maximum(top, zmr[t, 0:2, :])
    total = jnp.zeros_like(top)
    for t in range(nz):
        total = total + zmr[t, 2:4, :] * jnp.exp2(zmr[t, 0:2, :] - top)
    for t in range(nz):
        fz[t, 0:2, :] = jnp.exp2(zmr[t, 0:2, :] - top) / total

    first = z * (wide // PIECE) + x * pieces
    low = first // per_head
    acc[...] = jnp.zeros_like(acc)

    @pl.loop(0, nz)
    def _(i):
        t = far_peer(i)

        @pl.when(i > 0)
        def _():
            got(zr.at[t], z_r.at[t])

        for n in range(pieces):
            r = slice(n * PIECE, (n + 1) * PIECE)
            which = (first + n) // per_head - low
            acc[r, :] = acc[r, :] + zr[t, r, :].astype(F32) * fz[t, pl.ds(which, 1), :]

    for n in range(nc):
        attg[me, n] = acc[n * wrows : (n + 1) * wrows, :].astype(BF16)

    @pl.loop(1, near)
    def _(i):
        j = near_peer(i)
        send(attg.at[me], attg.at[me], at_s.at[j], at_r.at[me], near_id(j))

    @pl.loop(1, near)
    def _(i):
        j = near_peer(i)
        got(wbuf.at[j], w_r.at[j])

    @pl.loop(1, near)
    def _(i):
        j = near_peer(i)
        got(attg.at[j], at_r.at[j])

    share = nz // nc
    for cc in range(nc):
        product = None
        for xx in range(nx):
            for n in range(nc):
                term = lax.dot_general(
                    attg[xx * nc + cc, n], wbuf[xx * nc + n], (((0,), (0,)), ((), ())),
                    preferred_element_type=F32,
                )
                product = term if product is None else product + term
        pr[cc * share : (cc + 1) * share] = product.astype(BF16).reshape(share, -1, cols)

    @pl.loop(1, nz)
    def _(i):
        t = far_peer(i)
        send(pr.at[t], prr.at[z], p_s.at[t], p_r.at[z], {"z": t})

    prr[z] = pr[z]

    @pl.loop(1, nz)
    def _(i):
        t = far_peer(i)
        got(prr.at[t], p_r.at[t])

    sums = prr[0].astype(F32)
    for t in range(1, nz):
        sums = sums + prr[t].astype(F32)
    own = res_ref.shape[0]
    for j in range(near):
        fin[j] = sums[j * own : (j + 1) * own, :]

    @pl.loop(1, near)
    def _(i):
        j = near_peer(i)
        send(fin.at[j], finr.at[me], f_s.at[j], f_r.at[me], near_id(j))

    finr[me] = fin[me]

    @pl.loop(1, near)
    def _(i):
        j = near_peer(i)
        got(finr.at[j], f_r.at[j])

    even = (lax.broadcasted_iota(jnp.int32, (own, cols), 0) & 1) == 0
    for j in range(near):
        part = slice(j * cols, (j + 1) * cols)
        gates = jnp.where(even, gate_ref[:, part], 1.0 + null_ref[:, part])
        out_ref[:, part] = (res_ref[:, part].astype(F32) + gates * finr[j]).astype(BF16)

    @pl.loop(1, near)
    def _(i):
        j = near_peer(i)
        gone(ml_ref.at[0], ml_s.at[j])
        gone(wbuf.at[0], w_s.at[j])
        gone(attg.at[0], at_s.at[j])
        gone(fin.at[0], f_s.at[j])

    @pl.loop(0, nz)
    def _(t):
        gone(ra.at[pl.ds(0, wide)], a_s.at[t])
        gone(rel.at[0], o_s.at[t])
        gone(fin2.at[0], d_s.at[t])
        gone(relout.at[0], r_s.at[t])

    @pl.loop(1, nz)
    def _(i):
        t = far_peer(i)
        gone(zms.at[0], zm_s.at[t])
        gone(xs.at[0], z_s.at[t])
        gone(pr.at[0], p_s.at[t])


def join(numer, ml, weight, gate, null_gate, residual, places):
    nz, nx, nc = places
    near = nx * nc
    _, model_dim, half = numer.shape
    heads = ml.shape[2]
    wide = model_dim // nz
    blk = wide // nx
    cols = model_dim // near
    own = residual.shape[0]
    vmem = pl.BlockSpec(memory_space=pltpu.VMEM)
    dma = lambda n: pltpu.SemaphoreType.DMA((n,))
    band = 2 * half // nz
    blocks = pltpu.VMEM((nz, blk, half), BF16)
    scratch = [
        pltpu.VMEM((near, 2, heads, half), F32),
        pltpu.VMEM((2, heads, half), F32),
        pltpu.VMEM((2, heads, half), F32),
        pltpu.VMEM((model_dim, half), BF16),
        pltpu.VMEM((model_dim, half), BF16),
        blocks, blocks, blocks, blocks, blocks, blocks,
        pltpu.VMEM((nz, 8, half), F32),
        pltpu.VMEM((nz, 8, half), F32),
        pltpu.VMEM((nz, 8, half), F32),
        pltpu.VMEM((blk, half), F32),
        pltpu.VMEM((near, nc, weight.shape[0], half), BF16),
        pltpu.VMEM((near, weight.shape[0], cols), BF16),
        pltpu.VMEM((nz, band, cols), BF16),
        pltpu.VMEM((nz, band, cols), BF16),
        pltpu.VMEM((near, own, cols), F32),
        pltpu.VMEM((near, own, cols), F32),
    ]
    for size in (near, nz, nz, nz, nz, nz, nz, near, near, nz, near):
        scratch += [dma(size), dma(size)]
    return pl.pallas_call(
        functools.partial(join_kernel, places, min(4, nz)),
        out_shape=jax.ShapeDtypeStruct(residual.shape, BF16),
        in_specs=[vmem] * 6,
        out_specs=vmem,
        scratch_shapes=scratch,
        compiler_params=pltpu.CompilerParams(
            collective_id=0, has_side_effects=True, vmem_limit_bytes=48 << 20
        ),
        name="join",
    )(numer, ml, weight, gate, null_gate, residual)


def solution(mesh):
    places = (16, 4, 2)
    split = Mesh(mesh.devices.reshape(mesh.shape["groups"], *places), GROUPS_CTX)

    def on_device(
        queries, new_keys, new_values, cache_keys, cache_values, slot_of, cached, actions,
        action_table, null_gate, residual, out_weight,
    ):
        numer, ml, gate = attend(
            queries, new_keys, new_values, cache_keys, cache_values, slot_of, cached, actions,
            action_table, places,
        )
        return join(numer, ml, out_weight, gate, null_gate[None, :], residual, places)

    in_specs = (
        P("groups", None),
        P(GROUPS_CTX, None),
        P(GROUPS_CTX, None),
        P("groups", CTX, None, None),
        P("groups", CTX, None, None),
        P("groups"),
        P("groups"),
        P("groups", None),
        P(),
        P(),
        P(GROUPS_CTX, None),
        P(CTX, None),
    )
    return jax.shard_map(
        on_device, mesh=split, in_specs=in_specs, out_specs=P(GROUPS_CTX, None), check_vma=False
    )
```

```python
import functools
import math

import jax
import jax.numpy as jnp
from jax import lax
from jax.experimental import pallas as pl
from jax.experimental.pallas import tpu as pltpu
from jax.sharding import Mesh
from jax.sharding import PartitionSpec as P

HEAD = 128
PIECE = 16
CTX = ("z", "x", "core")
GROUPS_CTX = ("groups", "z", "x", "core")
MESH = pl.DeviceIdType.MESH
MASKED = -1e30
F32 = jnp.float32
BF16 = jnp.bfloat16
LAST = (((1,), (1,)), ((), ()))
FIRST = (((0,), (0,)), ((), ()))


def kernel(places, per_step, lag, *refs):
    (
        slot_ref, cached_ref, act_ref, q_ref, k_ref, v_ref, nk_ref, nv_ref, table_ref,
        w_ref, null_ref, res_ref, out_ref,
        bias, count, gate, away, home, ml, mlp, scale, joint, mlx, ratio,
        ra, d, rel, relout, fin1, fin2, xs, zr, zms, zmr, fz, acc,
        wn, att, attg, wbuf, pr, prr, fin, finr,
        ml_s, ml_r, mx_s, mx_r, a_s, a_r, o_s, o_r, d_s, d_r, r_s, r_r, z_s, z_r, zm_s, zm_r,
        wn_s, wn_r, at_s, at_r, w_s, w_r, p_s, p_r, f_s, f_r,
    ) = refs
    nz, nx, nc = places
    near = nx * nc
    z, x, c = (lax.axis_index(name) for name in CTX)
    me = x * nc + c
    other = 1 - c
    step = pl.program_id(0)
    steps = pl.num_programs(0)
    _, frames, tokens, _ = k_ref.shape
    sessions, acts = act_ref.shape
    rows = q_ref.shape[0]
    half = rows // nc
    session_rows = rows // sessions
    mine = sessions // nc
    slot_keys = frames * tokens
    keys = mine * slot_keys
    own = nk_ref.shape[0]
    model_dim = w_ref.shape[1]
    heads = model_dim // HEAD
    wide = model_dim // nz
    blk = wide // nx
    pieces = blk // PIECE
    per_head = HEAD // PIECE
    cols = model_dim // near
    wrows = w_ref.shape[0]
    pos = (z * nx + x) * nc + c
    parity = lax.rem(z, 2)
    twin = z + 1 - 2 * parity
    share = nz // nc
    barrier = pltpu.get_barrier_semaphore()

    def near_id(j):
        return {"x": j // nc, "core": lax.rem(j, nc)}

    def twin_id(j):
        return {"z": twin, "x": j // nc, "core": lax.rem(j, nc)}

    def near_peer(i):
        return lax.rem(me + i, near)

    def far_peer(i):
        return lax.rem(z + i, nz)

    def send(src, dst, ssem, rsem, where):
        pltpu.make_async_remote_copy(
            src_ref=src, dst_ref=dst, send_sem=ssem, recv_sem=rsem,
            device_id=where, device_id_type=MESH,
        ).start()

    def half_copy(ref, sem):
        return pltpu.make_async_remote_copy(
            src_ref=ref, dst_ref=ref, send_sem=sem, recv_sem=sem,
            device_id={"core": other}, device_id_type=MESH,
        )

    def got(ref, sem):
        half_copy(ref, sem).wait_recv()

    def gone(ref, sem):
        half_copy(ref, sem).wait_send()

    def greet(where):
        pl.semaphore_signal(barrier, inc=1, device_id=where, device_id_type=MESH)

    @pl.when(step == 0)
    def _():
        @pl.loop(1, nz)
        def _(i):
            greet({"z": far_peer(i)})

        @pl.loop(1, near)
        def _(i):
            greet(twin_id(near_peer(i)))
            greet(near_id(near_peer(i)))

        key = lax.broadcasted_iota(jnp.int32, (keys, half), 0)
        row = lax.broadcasted_iota(jnp.int32, (keys, half), 1)
        few_key = lax.broadcasted_iota(jnp.int32, (PIECE, half), 0)
        few_row = lax.broadcasted_iota(jnp.int32, (PIECE, half), 1)
        first = pos * own
        session = first // session_rows
        for part in range(nc):
            live = jnp.zeros((keys, half), jnp.int32)
            for s in range(mine):
                alive = cached_ref[part * mine + s] - pos * frames
                alive = jnp.clip(alive, 0, frames) * tokens
                here = (row >= s * session_rows) & (row < (s + 1) * session_rows)
                here = here & (key >= s * slot_keys) & (key < s * slot_keys + alive)
                live = jnp.where(here, 1, live)
            bias[part, 0:keys, :] = jnp.where(live == 1, 0.0, MASKED)
            low = session * session_rows - part * half
            good = (few_row >= low) & (few_row < low + session_rows) & (few_key < own)
            good = good & (((few_row + part * half - first - few_key) & 1) == 0)
            bias[part, keys : keys + PIECE, :] = jnp.where(good, 0.0, MASKED)
        vocab = table_ref.shape[0]
        lane = lax.broadcasted_iota(jnp.int32, (8, vocab), 1)
        sums = jnp.zeros((8, vocab), F32)
        for a in range(acts):
            sums = sums + jnp.where(lane == act_ref[session, a], 1.0, 0.0)
        count[...] = sums

    spot = lax.broadcasted_iota(jnp.int32, (PIECE, HEAD), 0)
    factor = math.log2(math.e) / math.sqrt(HEAD)

    def few(ref, part):
        values = jnp.zeros((PIECE, HEAD), F32)
        for j in range(own):
            values = jnp.where(spot == j, ref[j : j + 1, part].astype(F32), values)
        return values.astype(BF16)

    def taken(ref, extra, part, which):
        parts = []
        for s in range(mine):
            slot = slot_ref[which * mine + s]
            parts.append(ref[slot, :, :, part].reshape(slot_keys, HEAD))
        return jnp.concatenate(parts + [extra], 0)

    for i in range(per_step):
        part = slice(i * HEAD, (i + 1) * HEAD)
        head = step * per_step + i
        place = pl.ds(pl.multiple_of(head * HEAD, HEAD), HEAD)
        few_keys, few_values = few(nk_ref, part), few(nv_ref, part)
        for turn_of in range(nc):
            which = other if turn_of == 0 else c
            q = q_ref[pl.ds(pl.multiple_of(which * half, half), half), part]
            k = taken(k_ref, few_keys, part, which)
            v = taken(v_ref, few_values, part, which)
            s = lax.dot_general(k, q, LAST, preferred_element_type=F32)
            s = s * factor + bias[which]
            top = jnp.max(s, 0, keepdims=True)
            p = jnp.exp2(s - top)
            total = jnp.sum(p, 0, keepdims=True)
            numer = lax.dot_general(v, p.astype(BF16), FIRST, preferred_element_type=F32)
            if turn_of == 0:
                away[place, :] = numer.astype(BF16)
            else:
                home[place, :] = numer
            ml[turn_of, 0, pl.ds(head, 1), :] = top
            ml[turn_of, 1, pl.ds(head, 1), :] = total
    sums = jnp.dot(count[...].astype(BF16), table_ref[...], preferred_element_type=F32)
    width = per_step * HEAD
    spread = pl.ds(pl.multiple_of(step * width, width), width)
    gate[:, spread] = 1.0 + sums[0:1, :] / acts

    def turn(k):
        odd = lax.rem(k, 2)
        ahead = nz // 2 + odd * ((k + 1) // 2) - (1 - odd) * (k // 2)
        return lax.rem(z + ahead, nz)

    def ways(t):
        back = lax.rem(t, 2)
        ahead = lax.rem(x + 1 + (nx - 2) * back, nx)
        behind = lax.rem(x + nx - 1 - (nx - 2) * back, nx)
        return ahead, behind

    opposite = lax.rem(x + nx // 2, nx)

    def rows_of(t, xx):
        return pl.ds(pl.multiple_of(t * wide + xx * blk, PIECE), blk)

    def merge(k):
        t = turn(k)
        got(ra.at[pl.ds(pl.multiple_of(t * wide, PIECE), wide)], a_r.at[t])
        for i in range(wide // PIECE):
            g = t * (wide // PIECE) + i
            h = g // per_head
            r = pl.ds(pl.multiple_of(g * PIECE, PIECE), PIECE)
            here = home[r, :] * scale[0, pl.ds(h, 1), :]
            there = ra[r, :].astype(F32) * scale[1, pl.ds(h, 1), :]
            d[r, :] = (here + there).astype(BF16)
        ahead, behind = ways(t)
        send(d.at[rows_of(t, opposite)], rel.at[t], o_s.at[t], o_r.at[t], {"x": ahead})
        send(d.at[rows_of(t, behind)], fin2.at[t], d_s.at[t], d_r.at[t], {"x": behind})

    def scaled(t, xx, n):
        g = t * (wide // PIECE) + xx * pieces + n
        h = g // per_head
        r = pl.ds(pl.multiple_of(g * PIECE, PIECE), PIECE)
        return h, d[r, :].astype(F32) * ratio[x, pl.ds(h, 1), :]

    def relay(k):
        t = turn(k)
        ahead, behind = ways(t)
        got(rel.at[t], o_r.at[t])
        for n in range(pieces):
            h, value = scaled(t, ahead, n)
            r = slice(n * PIECE, (n + 1) * PIECE)
            value = value + rel[t, r, :].astype(F32) * ratio[behind, pl.ds(h, 1), :]
            relout[t, r, :] = value.astype(BF16)
        send(relout.at[t], fin1.at[t], r_s.at[t], r_r.at[t], {"x": ahead})

    def settle(k):
        t = turn(k)
        ahead, _ = ways(t)
        got(fin1.at[t], r_r.at[t])
        got(fin2.at[t], d_r.at[t])
        for n in range(pieces):
            h, value = scaled(t, x, n)
            r = slice(n * PIECE, (n + 1) * PIECE)
            value = value + fin2[t, r, :].astype(F32) * ratio[ahead, pl.ds(h, 1), :]
            xs[t, r, :] = (value + fin1[t, r, :].astype(F32)).astype(BF16)

        @pl.when(k < nz - 1)
        def _():
            send(xs.at[t], zr.at[z], z_s.at[t], z_r.at[z], {"z": t})

    def wpart(j):
        return pl.ds(pl.multiple_of(j * cols, cols), cols)

    def wplace(zz, j):
        return zz * near + j

    @pl.when(step == steps - 1)
    def _():
        pl.semaphore_wait(barrier, nz + 2 * near - 3)

        send(ml.at[0], mlp, ml_s, ml_r, {"core": other})

        @pl.loop(0, nz)
        def _(k):
            t = turn(k)
            part = pl.ds(pl.multiple_of(t * wide, PIECE), wide)
            send(away.at[part], ra.at[part], a_s.at[t], a_r.at[t], {"core": other})

        send(w_ref, wn, wn_s, wn_r, {"z": twin})

        got(mlp, ml_r)
        top = jnp.maximum(ml[1, 0], mlp[0])
        here, there = jnp.exp2(ml[1, 0] - top), jnp.exp2(mlp[0] - top)
        scale[0] = here
        scale[1] = there
        joint[0] = top
        joint[1] = ml[1, 1] * here + mlp[1] * there

        @pl.loop(1, nx)
        def _(i):
            xx = lax.rem(x + i, nx)
            send(joint, mlx.at[x], mx_s.at[xx], mx_r.at[x], {"x": xx})

        mlx[x] = joint[...]

        @pl.loop(0, lag)
        def _(k):
            merge(k)

        @pl.loop(1, nx)
        def _(i):
            xx = lax.rem(x + i, nx)
            got(mlx.at[xx], mx_r.at[xx])

        top = mlx[0, 0]
        for xx in range(1, nx):
            top = jnp.maximum(top, mlx[xx, 0])
        total = jnp.zeros_like(top)
        for xx in range(nx):
            part = jnp.exp2(mlx[xx, 0] - top)
            ratio[xx] = part
            total = total + mlx[xx, 1] * part
        scale2 = mlp
        scale2[0] = top
        scale2[1] = total

        @pl.loop(0, nz)
        def _(t):
            low = (t * (wide // PIECE) + x * pieces) // per_head
            high = jnp.minimum(low + 1, heads - 1)
            zms[t, 0:1, :] = scale2[0, pl.ds(low, 1), :]
            zms[t, 1:2, :] = scale2[0, pl.ds(high, 1), :]
            zms[t, 2:3, :] = scale2[1, pl.ds(low, 1), :]
            zms[t, 3:4, :] = scale2[1, pl.ds(high, 1), :]
            zms[t, 4:8, :] = jnp.zeros((4, half), F32)

        @pl.loop(1, nz)
        def _(i):
            t = far_peer(i)
            send(zms.at[t], zmr.at[z], zm_s.at[t], zm_r.at[z], {"z": t})

        @pl.loop(lag, nz + 2 * lag)
        def _(k):
            @pl.when(k < nz)
            def _():
                merge(k)

            @pl.when(k < nz + lag)
            def _():
                relay(k - lag)

            @pl.when(k >= 2 * lag)
            def _():
                settle(k - 2 * lag)

        got(wn, wn_r)

        @pl.loop(1, near)
        def _(i):
            j = near_peer(i)
            send(
                w_ref.at[:, wpart(j)], wbuf.at[wplace(parity, me)],
                w_s.at[0, j], w_r.at[0, me], near_id(j),
            )
            send(
                wn.at[:, wpart(j)], wbuf.at[wplace(1 - parity, me)],
                w_s.at[1, j], w_r.at[1, me], near_id(j),
            )

        wbuf[wplace(parity, me)] = w_ref[:, wpart(me)]
        wbuf[wplace(1 - parity, me)] = wn[:, wpart(me)]
        zr[z] = xs[z]
        zmr[z] = zms[z]

        @pl.loop(1, nz)
        def _(i):
            t = far_peer(i)
            got(zmr.at[t], zm_r.at[t])

        top = zmr[0, 0:2, :]
        for t in range(1, nz):
            top = jnp.maximum(top, zmr[t, 0:2, :])
        total = jnp.zeros_like(top)
        for t in range(nz):
            total = total + zmr[t, 2:4, :] * jnp.exp2(zmr[t, 0:2, :] - top)
        for t in range(nz):
            fz[t, 0:2, :] = jnp.exp2(zmr[t, 0:2, :] - top) / total

        first = z * (wide // PIECE) + x * pieces
        low = first // per_head
        acc[...] = jnp.zeros_like(acc)

        @pl.loop(0, nz)
        def _(i):
            t = far_peer(i)

            @pl.when(i > 0)
            def _():
                got(zr.at[t], z_r.at[t])

            for n in range(pieces):
                r = slice(n * PIECE, (n + 1) * PIECE)
                which = (first + n) // per_head - low
                acc[r, :] = acc[r, :] + zr[t, r, :].astype(F32) * fz[t, pl.ds(which, 1), :]

        for n in range(nc):
            att[n] = acc[n * wrows : (n + 1) * wrows, :].astype(BF16)

        goal = z - parity + c
        spot_of = parity * nx + x

        @pl.loop(0, near)
        def _(i):
            j = near_peer(i)

            @pl.when((goal != z) | (j != me))
            def _():
                send(
                    att, attg.at[spot_of], at_s.at[j], at_r.at[spot_of],
                    {"z": goal, "x": j // nc, "core": lax.rem(j, nc)},
                )

        @pl.when(goal == z)
        def _():
            attg[spot_of] = att[...]

        @pl.loop(1, near)
        def _(i):
            j = near_peer(i)
            got(wbuf.at[wplace(parity, j)], w_r.at[0, j])
            got(wbuf.at[wplace(1 - parity, j)], w_r.at[1, j])

        @pl.loop(0, near)
        def _(i):
            @pl.when((goal != z) | (i != spot_of))
            def _():
                got(attg.at[i], at_r.at[i])

        product = None
        for i in range(near):
            for n in range(nc):
                term = lax.dot_general(
                    attg[i, n], wbuf[i * nc + n], FIRST, preferred_element_type=F32
                )
                product = term if product is None else product + term
        pr[...] = product.astype(BF16).reshape(share, -1, cols)

        def ahead_of(i):
            return lax.rem(z + i, share)

        @pl.loop(0, share)
        def _(i):
            n = ahead_of(i)
            t = parity * share + n

            @pl.when(t != z)
            def _():
                send(pr.at[n], prr.at[z // nc], p_s.at[n], p_r.at[z // nc], {"z": t})

        @pl.when(z // share == parity)
        def _():
            prr[z // nc] = pr[lax.rem(z, share)]

        @pl.loop(0, share)
        def _(i):
            @pl.when(i * nc + z // share != z)
            def _():
                got(prr.at[i], p_r.at[i])

        sums = prr[0].astype(F32)
        for t in range(1, share):
            sums = sums + prr[t].astype(F32)
        for j in range(near):
            fin[j] = sums[j * own : (j + 1) * own, :]

        @pl.loop(1, near)
        def _(i):
            j = near_peer(i)
            send(fin.at[j], finr.at[me], f_s.at[j], f_r.at[me], near_id(j))

        finr[me] = fin[me]

        @pl.loop(1, near)
        def _(i):
            j = near_peer(i)
            got(finr.at[j], f_r.at[j])

        even = (lax.broadcasted_iota(jnp.int32, (own, cols), 0) & 1) == 0
        for j in range(near):
            part = slice(j * cols, (j + 1) * cols)
            gates = jnp.where(even, gate[:, part], 1.0 + null_ref[:, part])
            out_ref[:, part] = (res_ref[:, part].astype(F32) + gates * finr[j]).astype(BF16)

        gone(mlp, ml_s)
        gone(wn, wn_s)

        @pl.loop(1, nx)
        def _(i):
            gone(joint, mx_s.at[lax.rem(x + i, nx)])

        @pl.loop(1, near)
        def _(i):
            j = near_peer(i)
            gone(wbuf.at[0], w_s.at[0, j])
            gone(wbuf.at[0], w_s.at[1, j])
            gone(fin.at[0], f_s.at[j])

        @pl.loop(0, near)
        def _(j):
            @pl.when((goal != z) | (j != me))
            def _():
                gone(att, at_s.at[j])

        @pl.loop(0, share)
        def _(n):
            @pl.when(parity * share + n != z)
            def _():
                gone(pr.at[0], p_s.at[n])

        @pl.loop(0, nz)
        def _(t):
            gone(ra.at[pl.ds(0, wide)], a_s.at[t])
            gone(rel.at[0], o_s.at[t])
            gone(fin2.at[0], d_s.at[t])
            gone(relout.at[0], r_s.at[t])

        @pl.loop(1, nz)
        def _(i):
            t = far_peer(i)
            gone(zms.at[0], zm_s.at[t])
            gone(xs.at[0], z_s.at[t])


def run(places, slot_of, cached, actions, queries, keys, values, nk, nv, table, w, null, res):
    nz, nx, nc = places
    near = nx * nc
    rows, model_dim = queries.shape
    half = rows // nc
    heads = model_dim // HEAD
    per_step = 4 if heads % 4 == 0 else 1
    width = per_step * HEAD
    slots, frames, tokens, _ = keys.shape
    own = nk.shape[0]
    vocab = table.shape[0]
    wide = model_dim // nz
    blk = wide // nx
    cols = model_dim // near
    wrows = w.shape[0]
    share = nz // nc
    picked = slot_of.shape[0] // nc * frames * tokens + PIECE
    flat = lambda n: pl.BlockSpec((n, width), lambda i: (0, i))
    block = pl.BlockSpec((slots, frames, tokens, width), lambda i: (0, 0, 0, i))
    smem = pl.BlockSpec(memory_space=pltpu.SMEM)
    vmem = pl.BlockSpec(memory_space=pltpu.VMEM)
    dma = lambda *n: pltpu.SemaphoreType.DMA(n)
    f32 = lambda *n: pltpu.VMEM(n, F32)
    bf16 = lambda *n: pltpu.VMEM(n, BF16)
    scratch = [
        f32(nc, picked, half), f32(8, vocab), f32(1, model_dim),
        bf16(model_dim, half), f32(model_dim, half), f32(2, 2, heads, half),
        f32(2, heads, half), f32(2, heads, half), f32(2, heads, half),
        f32(nx, 2, heads, half), f32(nx, heads, half),
        bf16(model_dim, half), bf16(model_dim, half),
        *[bf16(nz, blk, half) for _ in range(6)],
        f32(nz, 8, half), f32(nz, 8, half), f32(nz, 8, half), f32(blk, half),
        bf16(wrows, model_dim), bf16(nc, wrows, half), bf16(near, nc, wrows, half),
        bf16(2 * near, wrows, cols),
        bf16(share, half // share, cols), bf16(share, half // share, cols),
        f32(near, own, cols), f32(near, own, cols),
    ]
    scratch += [pltpu.SemaphoreType.DMA, pltpu.SemaphoreType.DMA]
    for size in (nx, nz, nz, nz, nz, nz, nz):
        scratch += [dma(size), dma(size)]
    scratch += [pltpu.SemaphoreType.DMA, pltpu.SemaphoreType.DMA]
    scratch += [dma(near), dma(near), dma(2, near), dma(2, near)]
    scratch += [dma(share), dma(share), dma(near), dma(near)]
    return pl.pallas_call(
        functools.partial(kernel, places, per_step, min(4, nz)),
        grid=(heads // per_step,),
        in_specs=[smem] * 3 + [flat(rows), block, block, flat(own), flat(own), flat(vocab)] + [vmem] * 3,
        out_specs=vmem,
        out_shape=jax.ShapeDtypeStruct(res.shape, BF16),
        scratch_shapes=scratch,
        compiler_params=pltpu.CompilerParams(
            dimension_semantics=("arbitrary",), collective_id=0, has_side_effects=True,
            vmem_limit_bytes=52 << 20,
        ),
        name="rollout",
    )(slot_of, cached, actions, queries, keys, values, nk, nv, table, w, null, res)


def solution(mesh):
    places = (16, 4, 2)
    split = Mesh(mesh.devices.reshape(mesh.shape["groups"], *places), GROUPS_CTX)

    def on_device(
        queries, new_keys, new_values, cache_keys, cache_values, slot_of, cached, actions,
        action_table, null_gate, residual, out_weight,
    ):
        return run(
            places, slot_of, cached, actions, queries, cache_keys, cache_values, new_keys,
            new_values, action_table, out_weight, null_gate[None, :], residual,
        )

    in_specs = (
        P("groups", None),
        P(GROUPS_CTX, None),
        P(GROUPS_CTX, None),
        P("groups", CTX, None, None),
        P("groups", CTX, None, None),
        P("groups"),
        P("groups"),
        P("groups", None),
        P(),
        P(),
        P(GROUPS_CTX, None),
        P(CTX, None),
    )
    return jax.shard_map(
        on_device, mesh=split, in_specs=in_specs, out_specs=P(GROUPS_CTX, None), check_vma=False
    )
```

```python
import functools
import math

import jax
import jax.numpy as jnp
from jax import lax
from jax.experimental import pallas as pl
from jax.experimental.pallas import tpu as pltpu
from jax.sharding import Mesh
from jax.sharding import PartitionSpec as P

HEAD = 128
PIECE = 16
CTX = ("z", "x", "core")
GROUPS_CTX = ("groups", "z", "x", "core")
MESH = pl.DeviceIdType.MESH
MASKED = -1e30
F32 = jnp.float32
BF16 = jnp.bfloat16
LAST = (((1,), (1,)), ((), ()))
FIRST = (((0,), (0,)), ((), ()))


def kernel(places, per_step, lag, *refs):
    (
        slot_ref, cached_ref, act_ref, q_in, k_in, v_in, nk_in, nv_in, table_in,
        w_in, null_in, res_in, out_ref,
        q_ref, nk_ref, nv_ref, table_ref, w_ref, null_ref, res_ref, k_a, v_a, k_b, v_b, in_s, small_s,
        bias, count, gate, away, home, ml, mlp, scale, joint, mlx, ratio,
        ra, d, rel, relout, fin1, fin2, xs, zr, zms, zmr, fz, acc,
        wn, att, attg, wbuf, pr, prr, fin, finr,
        ml_s, ml_r, mx_s, mx_r, a_s, a_r, o_s, o_r, d_s, d_r, r_s, r_r, z_s, z_r, zm_s, zm_r,
        wn_s, wn_r, at_s, at_r, w_s, w_r, p_s, p_r, f_s, f_r,
    ) = refs
    nz, nx, nc = places
    near = nx * nc
    z, x, c = (lax.axis_index(name) for name in CTX)
    me = x * nc + c
    other = 1 - c
    _, frames, tokens, _ = k_in.shape
    sessions, acts = act_ref.shape
    rows = q_ref.shape[0]
    half = rows // nc
    session_rows = rows // sessions
    mine = sessions // nc
    slot_keys = frames * tokens
    keys = mine * slot_keys
    own = nk_ref.shape[0]
    model_dim = w_ref.shape[1]
    heads = model_dim // HEAD
    wide = model_dim // nz
    blk = wide // nx
    pieces = blk // PIECE
    per_head = HEAD // PIECE
    cols = model_dim // near
    wrows = w_ref.shape[0]
    pos = (z * nx + x) * nc + c
    parity = lax.rem(z, 2)
    twin = z + 1 - 2 * parity
    share = nz // nc
    width = per_step * HEAD
    steps = heads // per_step
    early = k_a.shape[3] // width
    spans = ((0, early, k_a, v_a), (early, steps, k_b, v_b))
    barrier = pltpu.get_barrier_semaphore()

    def near_id(j):
        return {"x": j // nc, "core": lax.rem(j, nc)}

    def twin_id(j):
        return {"z": twin, "x": j // nc, "core": lax.rem(j, nc)}

    def near_peer(i):
        return lax.rem(me + i, near)

    def far_peer(i):
        return lax.rem(z + i, nz)

    def send(src, dst, ssem, rsem, where):
        pltpu.make_async_remote_copy(
            src_ref=src, dst_ref=dst, send_sem=ssem, recv_sem=rsem,
            device_id=where, device_id_type=MESH,
        ).start()

    def half_copy(ref, sem):
        return pltpu.make_async_remote_copy(
            src_ref=ref, dst_ref=ref, send_sem=sem, recv_sem=sem,
            device_id={"core": other}, device_id_type=MESH,
        )

    def got(ref, sem):
        half_copy(ref, sem).wait_recv()

    def gone(ref, sem):
        half_copy(ref, sem).wait_send()

    def greet(where):
        pl.semaphore_signal(barrier, inc=1, device_id=where, device_id_type=MESH)

    @pl.loop(1, nz)
    def _(i):
        greet({"z": far_peer(i)})

    @pl.loop(1, near)
    def _(i):
        greet(twin_id(near_peer(i)))
        greet(near_id(near_peer(i)))

    smalls = (
        (nk_in, nk_ref), (nv_in, nv_ref), (w_in, w_ref), (table_in, table_ref),
        (null_in, null_ref), (res_in, res_ref),
    )

    def small(n):
        return pltpu.make_async_copy(*smalls[n], small_s.at[n])

    def chunk(step, begin, k_to, v_to):
        part = pl.ds(pl.multiple_of(step * width, width), width)
        into = pl.ds(pl.multiple_of((step - begin) * width, width), width)
        return (
            pltpu.make_async_copy(q_in.at[:, part], q_ref.at[:, part], in_s.at[0, step]),
            pltpu.make_async_copy(
                k_in.at[:, :, :, part], k_to.at[:, :, :, into], in_s.at[1, step]
            ),
            pltpu.make_async_copy(
                v_in.at[:, :, :, part], v_to.at[:, :, :, into], in_s.at[2, step]
            ),
        )

    small(0).start()
    small(1).start()

    for begin, end, k_to, v_to in spans:
        @pl.loop(begin, end)
        def _(step):
            for copy in chunk(step, begin, k_to, v_to):
                copy.start()

    for n in range(2, len(smalls)):
        small(n).start()

    key = lax.broadcasted_iota(jnp.int32, (keys, half), 0)
    row = lax.broadcasted_iota(jnp.int32, (keys, half), 1)
    few_key = lax.broadcasted_iota(jnp.int32, (PIECE, half), 0)
    few_row = lax.broadcasted_iota(jnp.int32, (PIECE, half), 1)
    first = pos * own
    session = first // session_rows
    for part in range(nc):
        live = jnp.zeros((keys, half), jnp.int32)
        for s in range(mine):
            alive = cached_ref[part * mine + s] - pos * frames
            alive = jnp.clip(alive, 0, frames) * tokens
            here = (row >= s * session_rows) & (row < (s + 1) * session_rows)
            here = here & (key >= s * slot_keys) & (key < s * slot_keys + alive)
            live = jnp.where(here, 1, live)
        bias[part, 0:keys, :] = jnp.where(live == 1, 0.0, MASKED)
        low = session * session_rows - part * half
        good = (few_row >= low) & (few_row < low + session_rows) & (few_key < own)
        good = good & (((few_row + part * half - first - few_key) & 1) == 0)
        bias[part, keys : keys + PIECE, :] = jnp.where(good, 0.0, MASKED)
    vocab = table_ref.shape[0]
    lane = lax.broadcasted_iota(jnp.int32, (8, vocab), 1)
    sums = jnp.zeros((8, vocab), F32)
    for a in range(acts):
        sums = sums + jnp.where(lane == act_ref[session, a], 1.0, 0.0)
    count[...] = sums

    spot = lax.broadcasted_iota(jnp.int32, (PIECE, HEAD), 0)
    factor = math.log2(math.e) / math.sqrt(HEAD)

    def few(ref, part):
        values = jnp.zeros((PIECE, HEAD), F32)
        for j in range(own):
            values = jnp.where(spot == j, ref[j : j + 1, part].astype(F32), values)
        return values.astype(BF16)

    def taken(ref, extra, part, which):
        parts = []
        for s in range(mine):
            slot = slot_ref[which * mine + s]
            parts.append(ref[slot, :, :, part].reshape(slot_keys, HEAD))
        return jnp.concatenate(parts + [extra], 0)

    small(0).wait()
    small(1).wait()

    def attend(step, i, begin, k_ref, v_ref):
        head = step * per_step + i
        place = pl.ds(pl.multiple_of(head * HEAD, HEAD), HEAD)
        part = place
        into = pl.ds(pl.multiple_of((head - begin * per_step) * HEAD, HEAD), HEAD)
        few_keys, few_values = few(nk_ref, part), few(nv_ref, part)
        for turn_of in range(nc):
            which = other if turn_of == 0 else c
            q = q_ref[pl.ds(pl.multiple_of(which * half, half), half), part]
            k = taken(k_ref, few_keys, into, which)
            v = taken(v_ref, few_values, into, which)
            s = lax.dot_general(k, q, LAST, preferred_element_type=F32)
            s = s * factor + bias[which]
            top = jnp.max(s, 0, keepdims=True)
            p = jnp.exp2(s - top)
            total = jnp.sum(p, 0, keepdims=True)
            numer = lax.dot_general(v, p.astype(BF16), FIRST, preferred_element_type=F32)
            if turn_of == 0:
                away[place, :] = numer.astype(BF16)
            else:
                home[place, :] = numer
            ml[turn_of, 0, pl.ds(head, 1), :] = top
            ml[turn_of, 1, pl.ds(head, 1), :] = total
    for begin, end, k_to, v_to in spans:
        @pl.loop(begin, end)
        def _(step):
            for copy in chunk(step, begin, k_to, v_to):
                copy.wait()

        @pl.loop(begin, end)
        def _(step):
            for i in range(per_step):
                attend(step, i, begin, k_to, v_to)

    small(2).wait()

    def turn(k):
        odd = lax.rem(k, 2)
        ahead = nz // 2 + odd * ((k + 1) // 2) - (1 - odd) * (k // 2)
        return lax.rem(z + ahead, nz)

    def ways(t):
        back = lax.rem(t, 2)
        ahead = lax.rem(x + 1 + (nx - 2) * back, nx)
        behind = lax.rem(x + nx - 1 - (nx - 2) * back, nx)
        return ahead, behind

    opposite = lax.rem(x + nx // 2, nx)

    def rows_of(t, xx):
        return pl.ds(pl.multiple_of(t * wide + xx * blk, PIECE), blk)

    def merge(k):
        t = turn(k)
        got(ra.at[pl.ds(pl.multiple_of(t * wide, PIECE), wide)], a_r.at[t])
        for i in range(wide // PIECE):
            g = t * (wide // PIECE) + i
            h = g // per_head
            r = pl.ds(pl.multiple_of(g * PIECE, PIECE), PIECE)
            here = home[r, :] * scale[0, pl.ds(h, 1), :]
            there = ra[r, :].astype(F32) * scale[1, pl.ds(h, 1), :]
            d[r, :] = (here + there).astype(BF16)
        ahead, behind = ways(t)
        send(d.at[rows_of(t, opposite)], rel.at[t], o_s.at[t], o_r.at[t], {"x": ahead})
        send(d.at[rows_of(t, behind)], fin2.at[t], d_s.at[t], d_r.at[t], {"x": behind})

    def scaled(t, xx, n):
        g = t * (wide // PIECE) + xx * pieces + n
        h = g // per_head
        r = pl.ds(pl.multiple_of(g * PIECE, PIECE), PIECE)
        return h, d[r, :].astype(F32) * ratio[x, pl.ds(h, 1), :]

    def relay(k):
        t = turn(k)
        ahead, behind = ways(t)
        got(rel.at[t], o_r.at[t])
        for n in range(pieces):
            h, value = scaled(t, ahead, n)
            r = slice(n * PIECE, (n + 1) * PIECE)
            value = value + rel[t, r, :].astype(F32) * ratio[behind, pl.ds(h, 1), :]
            relout[t, r, :] = value.astype(BF16)
        send(relout.at[t], fin1.at[t], r_s.at[t], r_r.at[t], {"x": ahead})

    def settle(k):
        t = turn(k)
        ahead, _ = ways(t)
        got(fin1.at[t], r_r.at[t])
        got(fin2.at[t], d_r.at[t])
        for n in range(pieces):
            h, value = scaled(t, x, n)
            r = slice(n * PIECE, (n + 1) * PIECE)
            value = value + fin2[t, r, :].astype(F32) * ratio[ahead, pl.ds(h, 1), :]
            xs[t, r, :] = (value + fin1[t, r, :].astype(F32)).astype(BF16)

        @pl.when(k < nz - 1)
        def _():
            send(xs.at[t], zr.at[z], z_s.at[t], z_r.at[z], {"z": t})

    def wpart(j):
        return pl.ds(pl.multiple_of(j * cols, cols), cols)

    def wplace(zz, j):
        return zz * near + j

    pl.semaphore_wait(barrier, nz + 2 * near - 3)

    send(ml.at[0], mlp, ml_s, ml_r, {"core": other})

    @pl.loop(0, nz)
    def _(k):
        t = turn(k)
        part = pl.ds(pl.multiple_of(t * wide, PIECE), wide)
        send(away.at[part], ra.at[part], a_s.at[t], a_r.at[t], {"core": other})

    send(w_ref, wn, wn_s, wn_r, {"z": twin})

    got(mlp, ml_r)
    top = jnp.maximum(ml[1, 0], mlp[0])
    here, there = jnp.exp2(ml[1, 0] - top), jnp.exp2(mlp[0] - top)
    scale[0] = here
    scale[1] = there
    joint[0] = top
    joint[1] = ml[1, 1] * here + mlp[1] * there

    @pl.loop(1, nx)
    def _(i):
        xx = lax.rem(x + i, nx)
        send(joint, mlx.at[x], mx_s.at[xx], mx_r.at[x], {"x": xx})

    mlx[x] = joint[...]

    @pl.loop(0, lag)
    def _(k):
        merge(k)

    @pl.loop(1, nx)
    def _(i):
        xx = lax.rem(x + i, nx)
        got(mlx.at[xx], mx_r.at[xx])

    top = mlx[0, 0]
    for xx in range(1, nx):
        top = jnp.maximum(top, mlx[xx, 0])
    total = jnp.zeros_like(top)
    for xx in range(nx):
        part = jnp.exp2(mlx[xx, 0] - top)
        ratio[xx] = part
        total = total + mlx[xx, 1] * part
    scale2 = mlp
    scale2[0] = top
    scale2[1] = total

    @pl.loop(0, nz)
    def _(t):
        low = (t * (wide // PIECE) + x * pieces) // per_head
        high = jnp.minimum(low + 1, heads - 1)
        zms[t, 0:1, :] = scale2[0, pl.ds(low, 1), :]
        zms[t, 1:2, :] = scale2[0, pl.ds(high, 1), :]
        zms[t, 2:3, :] = scale2[1, pl.ds(low, 1), :]
        zms[t, 3:4, :] = scale2[1, pl.ds(high, 1), :]
        zms[t, 4:8, :] = jnp.zeros((4, half), F32)

    @pl.loop(1, nz)
    def _(i):
        t = far_peer(i)
        send(zms.at[t], zmr.at[z], zm_s.at[t], zm_r.at[z], {"z": t})

    @pl.loop(lag, nz + 2 * lag)
    def _(k):
        @pl.when(k < nz)
        def _():
            merge(k)

        @pl.when(k < nz + lag)
        def _():
            relay(k - lag)

        @pl.when(k >= 2 * lag)
        def _():
            settle(k - 2 * lag)

    got(wn, wn_r)

    @pl.loop(1, near)
    def _(i):
        j = near_peer(i)
        send(
            w_ref.at[:, wpart(j)], wbuf.at[wplace(parity, me)],
            w_s.at[0, j], w_r.at[0, me], near_id(j),
        )
        send(
            wn.at[:, wpart(j)], wbuf.at[wplace(1 - parity, me)],
            w_s.at[1, j], w_r.at[1, me], near_id(j),
        )

    wbuf[wplace(parity, me)] = w_ref[:, wpart(me)]
    wbuf[wplace(1 - parity, me)] = wn[:, wpart(me)]
    zr[z] = xs[z]
    zmr[z] = zms[z]

    @pl.loop(1, nz)
    def _(i):
        t = far_peer(i)
        got(zmr.at[t], zm_r.at[t])

    top = zmr[0, 0:2, :]
    for t in range(1, nz):
        top = jnp.maximum(top, zmr[t, 0:2, :])
    total = jnp.zeros_like(top)
    for t in range(nz):
        total = total + zmr[t, 2:4, :] * jnp.exp2(zmr[t, 0:2, :] - top)
    for t in range(nz):
        fz[t, 0:2, :] = jnp.exp2(zmr[t, 0:2, :] - top) / total

    first = z * (wide // PIECE) + x * pieces
    low = first // per_head
    acc[...] = jnp.zeros_like(acc)

    @pl.loop(0, nz)
    def _(i):
        t = far_peer(i)

        @pl.when(i > 0)
        def _():
            got(zr.at[t], z_r.at[t])

        for n in range(pieces):
            r = slice(n * PIECE, (n + 1) * PIECE)
            which = (first + n) // per_head - low
            acc[r, :] = acc[r, :] + zr[t, r, :].astype(F32) * fz[t, pl.ds(which, 1), :]

    for n in range(nc):
        att[n] = acc[n * wrows : (n + 1) * wrows, :].astype(BF16)

    goal = z - parity + c
    spot_of = parity * nx + x

    @pl.loop(0, near)
    def _(i):
        j = near_peer(i)

        @pl.when((goal != z) | (j != me))
        def _():
            send(
                att, attg.at[spot_of], at_s.at[j], at_r.at[spot_of],
                {"z": goal, "x": j // nc, "core": lax.rem(j, nc)},
            )

    @pl.when(goal == z)
    def _():
        attg[spot_of] = att[...]

    @pl.loop(1, near)
    def _(i):
        j = near_peer(i)
        got(wbuf.at[wplace(parity, j)], w_r.at[0, j])
        got(wbuf.at[wplace(1 - parity, j)], w_r.at[1, j])

    @pl.loop(0, near)
    def _(i):
        @pl.when((goal != z) | (i != spot_of))
        def _():
            got(attg.at[i], at_r.at[i])

    product = None
    for i in range(near):
        for n in range(nc):
            term = lax.dot_general(
                attg[i, n], wbuf[i * nc + n], FIRST, preferred_element_type=F32
            )
            product = term if product is None else product + term
    pr[...] = product.astype(BF16).reshape(share, -1, cols)

    def ahead_of(i):
        odd = lax.rem(i, 2)
        skew = odd * ((i + 1) // 2) + (1 - odd) * (share - i // 2)
        near_half = jnp.where(z // share == parity, share // 2, 0)
        return lax.rem(z + near_half + skew, share)

    @pl.loop(0, share)
    def _(i):
        n = ahead_of(i)
        t = parity * share + n

        @pl.when(t != z)
        def _():
            send(pr.at[n], prr.at[z // nc], p_s.at[n], p_r.at[z // nc], {"z": t})

    @pl.when(z // share == parity)
    def _():
        prr[z // nc] = pr[lax.rem(z, share)]

    small(3).wait()
    small(4).wait()
    small(5).wait()

    @pl.loop(0, steps)
    def _(step):
        spread = pl.ds(pl.multiple_of(step * width, width), width)
        sums = jnp.dot(count[...].astype(BF16), table_ref[:, spread], preferred_element_type=F32)
        gate[:, spread] = 1.0 + sums[0:1, :] / acts

    @pl.loop(0, share)
    def _(i):
        @pl.when(i * nc + z // share != z)
        def _():
            got(prr.at[i], p_r.at[i])

    sums = prr[0].astype(F32)
    for t in range(1, share):
        sums = sums + prr[t].astype(F32)
    for j in range(near):
        fin[j] = sums[j * own : (j + 1) * own, :]

    @pl.loop(1, near)
    def _(i):
        j = near_peer(i)
        send(fin.at[j], finr.at[me], f_s.at[j], f_r.at[me], near_id(j))

    finr[me] = fin[me]

    @pl.loop(1, near)
    def _(i):
        j = near_peer(i)
        got(finr.at[j], f_r.at[j])

    even = (lax.broadcasted_iota(jnp.int32, (own, cols), 0) & 1) == 0
    for j in range(near):
        part = slice(j * cols, (j + 1) * cols)
        gates = jnp.where(even, gate[:, part], 1.0 + null_ref[:, part])
        out_ref[:, part] = (res_ref[:, part].astype(F32) + gates * finr[j]).astype(BF16)

    gone(mlp, ml_s)
    gone(wn, wn_s)

    @pl.loop(1, nx)
    def _(i):
        gone(joint, mx_s.at[lax.rem(x + i, nx)])

    @pl.loop(1, near)
    def _(i):
        j = near_peer(i)
        gone(wbuf.at[0], w_s.at[0, j])
        gone(wbuf.at[0], w_s.at[1, j])
        gone(fin.at[0], f_s.at[j])

    @pl.loop(0, near)
    def _(j):
        @pl.when((goal != z) | (j != me))
        def _():
            gone(att, at_s.at[j])

    @pl.loop(0, share)
    def _(n):
        @pl.when(parity * share + n != z)
        def _():
            gone(pr.at[0], p_s.at[n])

    @pl.loop(0, nz)
    def _(t):
        gone(ra.at[pl.ds(0, wide)], a_s.at[t])
        gone(rel.at[0], o_s.at[t])
        gone(fin2.at[0], d_s.at[t])
        gone(relout.at[0], r_s.at[t])

    @pl.loop(1, nz)
    def _(i):
        t = far_peer(i)
        gone(zms.at[0], zm_s.at[t])
        gone(xs.at[0], z_s.at[t])


def run(places, slot_of, cached, actions, queries, keys, values, nk, nv, table, w, null, res):
    nz, nx, nc = places
    near = nx * nc
    rows, model_dim = queries.shape
    half = rows // nc
    heads = model_dim // HEAD
    per_step = 4 if heads % 4 == 0 else 1
    _, frames, tokens, _ = keys.shape
    own = nk.shape[0]
    vocab = table.shape[0]
    wide = model_dim // nz
    blk = wide // nx
    cols = model_dim // near
    wrows = w.shape[0]
    share = nz // nc
    picked = slot_of.shape[0] // nc * frames * tokens + PIECE
    smem = pl.BlockSpec(memory_space=pltpu.SMEM)
    vmem = pl.BlockSpec(memory_space=pltpu.VMEM)
    away = pl.BlockSpec(memory_space=pl.ANY)
    dma = lambda *n: pltpu.SemaphoreType.DMA(n)
    f32 = lambda *n: pltpu.VMEM(n, F32)
    bf16 = lambda *n: pltpu.VMEM(n, BF16)
    large = (queries, nk, nv, table, w, null, res)
    scratch = [pltpu.VMEM(value.shape, value.dtype) for value in large]
    steps = heads // per_step
    early = max(1, steps // 5)
    for size in (early, early, steps - early, steps - early):
        scratch.append(bf16(*keys.shape[:3], size * per_step * HEAD))
    scratch += [dma(3, heads // per_step), dma(6)]
    scratch += [
        f32(nc, picked, half), f32(8, vocab), f32(1, model_dim),
        bf16(model_dim, half), f32(model_dim, half), f32(2, 2, heads, half),
        f32(2, heads, half), f32(2, heads, half), f32(2, heads, half),
        f32(nx, 2, heads, half), f32(nx, heads, half),
        bf16(model_dim, half), bf16(model_dim, half),
        *[bf16(nz, blk, half) for _ in range(6)],
        f32(nz, 8, half), f32(nz, 8, half), f32(nz, 8, half), f32(blk, half),
        bf16(wrows, model_dim), bf16(nc, wrows, half), bf16(near, nc, wrows, half),
        bf16(2 * near, wrows, cols),
        bf16(share, half // share, cols), bf16(share, half // share, cols),
        f32(near, own, cols), f32(near, own, cols),
    ]
    scratch += [pltpu.SemaphoreType.DMA, pltpu.SemaphoreType.DMA]
    for size in (nx, nz, nz, nz, nz, nz, nz):
        scratch += [dma(size), dma(size)]
    scratch += [pltpu.SemaphoreType.DMA, pltpu.SemaphoreType.DMA]
    scratch += [dma(near), dma(near), dma(2, near), dma(2, near)]
    scratch += [dma(share), dma(share), dma(near), dma(near)]
    return pl.pallas_call(
        functools.partial(kernel, places, per_step, min(4, nz)),
        in_specs=[smem] * 3 + [away] * 9,
        out_specs=vmem,
        out_shape=jax.ShapeDtypeStruct(res.shape, BF16),
        scratch_shapes=scratch,
        compiler_params=pltpu.CompilerParams(
            collective_id=0, has_side_effects=True, vmem_limit_bytes=67_043_328
        ),
        name="rollout",
    )(slot_of, cached, actions, queries, keys, values, nk, nv, table, w, null, res)


def solution(mesh):
    places = (16, 4, 2)
    split = Mesh(mesh.devices.reshape(mesh.shape["groups"], *places), GROUPS_CTX)

    def on_device(
        queries, new_keys, new_values, cache_keys, cache_values, slot_of, cached, actions,
        action_table, null_gate, residual, out_weight,
    ):
        return run(
            places, slot_of, cached, actions, queries, cache_keys, cache_values, new_keys,
            new_values, action_table, out_weight, null_gate[None, :], residual,
        )

    in_specs = (
        P("groups", None),
        P(GROUPS_CTX, None),
        P(GROUPS_CTX, None),
        P("groups", CTX, None, None),
        P("groups", CTX, None, None),
        P("groups"),
        P("groups"),
        P("groups", None),
        P(),
        P(),
        P(GROUPS_CTX, None),
        P(CTX, None),
    )
    return jax.shard_map(
        on_device, mesh=split, in_specs=in_specs, out_specs=P(GROUPS_CTX, None), check_vma=False
    )
```

```python
import functools
import math

import jax
import jax.numpy as jnp
from jax import lax
from jax.experimental import pallas as pl
from jax.experimental.pallas import tpu as pltpu
from jax.sharding import Mesh
from jax.sharding import PartitionSpec as P

HEAD = 128
PIECE = 16
CTX = ("z", "x", "core")
GROUPS_CTX = ("groups", "z", "x", "core")
MESH = pl.DeviceIdType.MESH
MASKED = -1e30
F32 = jnp.float32
BF16 = jnp.bfloat16
LAST = (((1,), (1,)), ((), ()))
FIRST = (((0,), (0,)), ((), ()))


def kernel(places, per_step, lag, *refs):
    (
        slot_ref, cached_ref, act_ref, q_in, k_in, v_in, nk_in, nv_in, table_in,
        w_in, null_in, res_in, out_ref,
        q_ref, nk_ref, nv_ref, table_ref, w_ref, null_ref, res_ref, k_ref, v_ref, in_s, small_s,
        bias, count, gate, away, home, ml, mlp, scale, joint, mlx, ratio,
        ra, d, rel, relout, fin1, fin2, xs, zr, zms, zmr, fz, acc,
        wn, att, attg, wbuf, pr, prr, fin, finr,
        ml_s, ml_r, mx_s, mx_r, a_s, a_r, o_s, o_r, d_s, d_r, r_s, r_r, z_s, z_r, zm_s, zm_r,
        wn_s, wn_r, at_s, at_r, w_s, w_r, p_s, p_r, f_s, f_r,
    ) = refs
    nz, nx, nc = places
    near = nx * nc
    z, x, c = (lax.axis_index(name) for name in CTX)
    me = x * nc + c
    other = 1 - c
    _, frames, tokens, _ = k_in.shape
    sessions, acts = act_ref.shape
    rows = q_ref.shape[0]
    half = rows // nc
    session_rows = rows // sessions
    mine = sessions // nc
    slot_keys = frames * tokens
    keys = mine * slot_keys
    own = nk_ref.shape[0]
    model_dim = w_ref.shape[1]
    heads = model_dim // HEAD
    wide = model_dim // nz
    blk = wide // nx
    pieces = blk // PIECE
    per_head = HEAD // PIECE
    cols = model_dim // near
    wrows = w_ref.shape[0]
    pos = (z * nx + x) * nc + c
    parity = lax.rem(z, 2)
    twin = z + 1 - 2 * parity
    share = nz // nc
    width = per_step * HEAD
    steps = heads // per_step
    barrier = pltpu.get_barrier_semaphore()

    def near_id(j):
        return {"x": j // nc, "core": lax.rem(j, nc)}

    def twin_id(j):
        return {"z": twin, "x": j // nc, "core": lax.rem(j, nc)}

    def near_peer(i):
        return lax.rem(me + i, near)

    def far_peer(i):
        return lax.rem(z + i, nz)

    def send(src, dst, ssem, rsem, where):
        pltpu.make_async_remote_copy(
            src_ref=src, dst_ref=dst, send_sem=ssem, recv_sem=rsem,
            device_id=where, device_id_type=MESH,
        ).start()

    def half_copy(ref, sem):
        return pltpu.make_async_remote_copy(
            src_ref=ref, dst_ref=ref, send_sem=sem, recv_sem=sem,
            device_id={"core": other}, device_id_type=MESH,
        )

    def got(ref, sem):
        half_copy(ref, sem).wait_recv()

    def gone(ref, sem):
        half_copy(ref, sem).wait_send()

    def greet(where):
        pl.semaphore_signal(barrier, inc=1, device_id=where, device_id_type=MESH)

    @pl.loop(1, nz)
    def _(i):
        greet({"z": far_peer(i)})

    @pl.loop(1, near)
    def _(i):
        greet(twin_id(near_peer(i)))
        greet(near_id(near_peer(i)))

    smalls = (
        (nk_in, nk_ref), (nv_in, nv_ref), (w_in, w_ref), (table_in, table_ref),
        (null_in, null_ref), (res_in, res_ref),
    )

    def small(n):
        return pltpu.make_async_copy(*smalls[n], small_s.at[n])

    def load(n):
        band = rows // k_in.shape[0]
        part = pl.ds(pl.multiple_of(n * band, band), band)
        return (
            pltpu.make_async_copy(k_in.at[n], k_ref.at[n], in_s.at[0, n]),
            pltpu.make_async_copy(q_in.at[part], q_ref.at[part], in_s.at[1, n]),
            pltpu.make_async_copy(v_in.at[n], v_ref.at[n], in_s.at[2, n]),
        )

    small(0).start()
    small(1).start()

    @pl.loop(0, k_in.shape[0])
    def _(n):
        for copy in load(n):
            copy.start()

    key = lax.broadcasted_iota(jnp.int32, (keys, half), 0)
    row = lax.broadcasted_iota(jnp.int32, (keys, half), 1)
    few_key = lax.broadcasted_iota(jnp.int32, (PIECE, half), 0)
    few_row = lax.broadcasted_iota(jnp.int32, (PIECE, half), 1)
    first = pos * own
    session = first // session_rows
    for part in range(nc):
        live = jnp.zeros((keys, half), jnp.int32)
        for s in range(mine):
            alive = cached_ref[part * mine + s] - pos * frames
            alive = jnp.clip(alive, 0, frames) * tokens
            here = (row >= s * session_rows) & (row < (s + 1) * session_rows)
            here = here & (key >= s * slot_keys) & (key < s * slot_keys + alive)
            live = jnp.where(here, 1, live)
        bias[part, 0:keys, :] = jnp.where(live == 1, 0.0, MASKED)
        low = session * session_rows - part * half
        good = (few_row >= low) & (few_row < low + session_rows) & (few_key < own)
        good = good & (((few_row + part * half - first - few_key) & 1) == 0)
        bias[part, keys : keys + PIECE, :] = jnp.where(good, 0.0, MASKED)
    vocab = table_ref.shape[0]
    lane = lax.broadcasted_iota(jnp.int32, (8, vocab), 1)
    sums = jnp.zeros((8, vocab), F32)
    for a in range(acts):
        sums = sums + jnp.where(lane == act_ref[session, a], 1.0, 0.0)
    count[...] = sums

    spot = lax.broadcasted_iota(jnp.int32, (PIECE, HEAD), 0)
    factor = math.log2(math.e) / math.sqrt(HEAD)

    def few(ref, part):
        values = jnp.zeros((PIECE, HEAD), F32)
        for j in range(own):
            values = jnp.where(spot == j, ref[j : j + 1, part].astype(F32), values)
        return values.astype(BF16)

    def taken(ref, extra, part, which):
        parts = []
        for s in range(mine):
            slot = slot_ref[which * mine + s]
            parts.append(ref[slot, :, :, part].reshape(slot_keys, HEAD))
        return jnp.concatenate(parts + [extra], 0)

    small(0).wait()
    small(1).wait()

    def attend(step):
        work = []
        for i in range(per_step):
            head = step * per_step + i
            part = pl.ds(pl.multiple_of(head * HEAD, HEAD), HEAD)
            few_keys = few(nk_ref, part)
            for which in (other, c):
                q = q_ref[pl.ds(pl.multiple_of(which * half, half), half), part]
                k = taken(k_ref, few_keys, part, which)
                s = lax.dot_general(k, q, LAST, preferred_element_type=F32)
                work.append((head, part, which, s))
        ready = []
        for head, part, which, s in work:
            s = s * factor + bias[which]
            top = jnp.max(s, 0, keepdims=True)
            p = jnp.exp2(s - top)
            total = jnp.sum(p, 0, keepdims=True)
            first = 0 if which is other else 1
            ml[first, 0, pl.ds(head, 1), :] = top
            ml[first, 1, pl.ds(head, 1), :] = total
            ready.append((part, which, p.astype(BF16)))
        for part, which, p in ready:
            v = taken(v_ref, few(nv_ref, part), part, which)
            numer = lax.dot_general(v, p, FIRST, preferred_element_type=F32)
            if which is other:
                away[part, :] = numer.astype(BF16)
            else:
                home[part, :] = numer

    for copy in [copy for n in range(k_in.shape[0]) for copy in load(n)]:
        copy.wait()

    for n in range(2, len(smalls)):
        small(n).start()

    @pl.loop(0, steps)
    def _(step):
        attend(step)

    small(2).wait()

    def turn(k):
        odd = lax.rem(k, 2)
        ahead = nz // 2 + odd * ((k + 1) // 2) - (1 - odd) * (k // 2)
        return lax.rem(z + ahead, nz)

    def ways(t):
        back = lax.rem(t, 2)
        ahead = lax.rem(x + 1 + (nx - 2) * back, nx)
        behind = lax.rem(x + nx - 1 - (nx - 2) * back, nx)
        return ahead, behind

    opposite = lax.rem(x + nx // 2, nx)

    def rows_of(t, xx):
        return pl.ds(pl.multiple_of(t * wide + xx * blk, PIECE), blk)

    def merge(k):
        t = turn(k)
        got(ra.at[pl.ds(pl.multiple_of(t * wide, PIECE), wide)], a_r.at[t])
        for i in range(wide // PIECE):
            g = t * (wide // PIECE) + i
            h = g // per_head
            r = pl.ds(pl.multiple_of(g * PIECE, PIECE), PIECE)
            here = home[r, :] * scale[0, pl.ds(h, 1), :]
            there = ra[r, :].astype(F32) * scale[1, pl.ds(h, 1), :]
            d[r, :] = (here + there).astype(BF16)
        ahead, behind = ways(t)
        send(d.at[rows_of(t, opposite)], rel.at[t], o_s.at[t], o_r.at[t], {"x": ahead})
        send(d.at[rows_of(t, behind)], fin2.at[t], d_s.at[t], d_r.at[t], {"x": behind})

    def scaled(t, xx, n):
        g = t * (wide // PIECE) + xx * pieces + n
        h = g // per_head
        r = pl.ds(pl.multiple_of(g * PIECE, PIECE), PIECE)
        return h, d[r, :].astype(F32) * ratio[x, pl.ds(h, 1), :]

    def relay(k):
        t = turn(k)
        ahead, behind = ways(t)
        got(rel.at[t], o_r.at[t])
        for n in range(pieces):
            h, value = scaled(t, ahead, n)
            r = slice(n * PIECE, (n + 1) * PIECE)
            value = value + rel[t, r, :].astype(F32) * ratio[behind, pl.ds(h, 1), :]
            relout[t, r, :] = value.astype(BF16)
        send(relout.at[t], fin1.at[t], r_s.at[t], r_r.at[t], {"x": ahead})

    def settle(k):
        t = turn(k)
        ahead, _ = ways(t)
        got(fin1.at[t], r_r.at[t])
        got(fin2.at[t], d_r.at[t])
        for n in range(pieces):
            h, value = scaled(t, x, n)
            r = slice(n * PIECE, (n + 1) * PIECE)
            value = value + fin2[t, r, :].astype(F32) * ratio[ahead, pl.ds(h, 1), :]
            xs[t, r, :] = (value + fin1[t, r, :].astype(F32)).astype(BF16)

        @pl.when(k < nz - 1)
        def _():
            send(xs.at[t], zr.at[z], z_s.at[t], z_r.at[z], {"z": t})

    def wpart(j):
        return pl.ds(pl.multiple_of(j * cols, cols), cols)

    def wplace(zz, j):
        return zz * near + j

    pl.semaphore_wait(barrier, nz + 2 * near - 3)

    send(ml.at[0], mlp, ml_s, ml_r, {"core": other})

    @pl.loop(0, nz)
    def _(k):
        t = turn(k)
        part = pl.ds(pl.multiple_of(t * wide, PIECE), wide)
        send(away.at[part], ra.at[part], a_s.at[t], a_r.at[t], {"core": other})

    send(w_ref, wn, wn_s, wn_r, {"z": twin})

    got(mlp, ml_r)
    top = jnp.maximum(ml[1, 0], mlp[0])
    here, there = jnp.exp2(ml[1, 0] - top), jnp.exp2(mlp[0] - top)
    scale[0] = here
    scale[1] = there
    joint[0] = top
    joint[1] = ml[1, 1] * here + mlp[1] * there

    @pl.loop(1, nx)
    def _(i):
        xx = lax.rem(x + i, nx)
        send(joint, mlx.at[x], mx_s.at[xx], mx_r.at[x], {"x": xx})

    mlx[x] = joint[...]

    @pl.loop(0, lag)
    def _(k):
        merge(k)

    @pl.loop(1, nx)
    def _(i):
        xx = lax.rem(x + i, nx)
        got(mlx.at[xx], mx_r.at[xx])

    top = mlx[0, 0]
    for xx in range(1, nx):
        top = jnp.maximum(top, mlx[xx, 0])
    total = jnp.zeros_like(top)
    for xx in range(nx):
        part = jnp.exp2(mlx[xx, 0] - top)
        ratio[xx] = part
        total = total + mlx[xx, 1] * part
    scale2 = mlp
    scale2[0] = top
    scale2[1] = total

    @pl.loop(0, nz)
    def _(t):
        low = (t * (wide // PIECE) + x * pieces) // per_head
        high = jnp.minimum(low + 1, heads - 1)
        zms[t, 0:1, :] = scale2[0, pl.ds(low, 1), :]
        zms[t, 1:2, :] = scale2[0, pl.ds(high, 1), :]
        zms[t, 2:3, :] = scale2[1, pl.ds(low, 1), :]
        zms[t, 3:4, :] = scale2[1, pl.ds(high, 1), :]
        zms[t, 4:8, :] = jnp.zeros((4, half), F32)

    @pl.loop(1, nz)
    def _(i):
        t = far_peer(i)
        send(zms.at[t], zmr.at[z], zm_s.at[t], zm_r.at[z], {"z": t})

    @pl.loop(lag, nz + 2 * lag)
    def _(k):
        @pl.when(k < nz)
        def _():
            merge(k)

        @pl.when(k < nz + lag)
        def _():
            relay(k - lag)

        @pl.when(k >= 2 * lag)
        def _():
            settle(k - 2 * lag)

    got(wn, wn_r)

    @pl.loop(1, near)
    def _(i):
        j = near_peer(i)
        send(
            w_ref.at[:, wpart(j)], wbuf.at[wplace(parity, me)],
            w_s.at[0, j], w_r.at[0, me], near_id(j),
        )
        send(
            wn.at[:, wpart(j)], wbuf.at[wplace(1 - parity, me)],
            w_s.at[1, j], w_r.at[1, me], near_id(j),
        )

    wbuf[wplace(parity, me)] = w_ref[:, wpart(me)]
    wbuf[wplace(1 - parity, me)] = wn[:, wpart(me)]
    zr[z] = xs[z]
    zmr[z] = zms[z]

    @pl.loop(1, nz)
    def _(i):
        t = far_peer(i)
        got(zmr.at[t], zm_r.at[t])

    top = zmr[0, 0:2, :]
    for t in range(1, nz):
        top = jnp.maximum(top, zmr[t, 0:2, :])
    total = jnp.zeros_like(top)
    for t in range(nz):
        total = total + zmr[t, 2:4, :] * jnp.exp2(zmr[t, 0:2, :] - top)
    for t in range(nz):
        fz[t, 0:2, :] = jnp.exp2(zmr[t, 0:2, :] - top) / total

    first = z * (wide // PIECE) + x * pieces
    low = first // per_head
    acc[...] = jnp.zeros_like(acc)

    @pl.loop(0, nz)
    def _(i):
        t = far_peer(i)

        @pl.when(i > 0)
        def _():
            got(zr.at[t], z_r.at[t])

        for n in range(pieces):
            r = slice(n * PIECE, (n + 1) * PIECE)
            which = (first + n) // per_head - low
            acc[r, :] = acc[r, :] + zr[t, r, :].astype(F32) * fz[t, pl.ds(which, 1), :]

    for n in range(nc):
        att[n] = acc[n * wrows : (n + 1) * wrows, :].astype(BF16)

    goal = z - parity + c
    spot_of = parity * nx + x

    @pl.loop(0, near)
    def _(i):
        j = near_peer(i)

        @pl.when((goal != z) | (j != me))
        def _():
            send(
                att, attg.at[spot_of], at_s.at[j], at_r.at[spot_of],
                {"z": goal, "x": j // nc, "core": lax.rem(j, nc)},
            )

    @pl.when(goal == z)
    def _():
        attg[spot_of] = att[...]

    @pl.loop(1, near)
    def _(i):
        j = near_peer(i)
        got(wbuf.at[wplace(parity, j)], w_r.at[0, j])
        got(wbuf.at[wplace(1 - parity, j)], w_r.at[1, j])

    @pl.loop(0, near)
    def _(i):
        @pl.when((goal != z) | (i != spot_of))
        def _():
            got(attg.at[i], at_r.at[i])

    product = None
    for i in range(near):
        for n in range(nc):
            term = lax.dot_general(
                attg[i, n], wbuf[i * nc + n], FIRST, preferred_element_type=F32
            )
            product = term if product is None else product + term
    pr[...] = product.astype(BF16).reshape(share, -1, cols)

    def ahead_of(i):
        odd = lax.rem(i, 2)
        skew = odd * ((i + 1) // 2) + (1 - odd) * (share - i // 2)
        near_half = jnp.where(z // share == parity, share // 2, 0)
        return lax.rem(z + near_half + skew, share)

    @pl.loop(0, share)
    def _(i):
        n = ahead_of(i)
        t = parity * share + n

        @pl.when(t != z)
        def _():
            send(pr.at[n], prr.at[z // nc], p_s.at[n], p_r.at[z // nc], {"z": t})

    @pl.when(z // share == parity)
    def _():
        prr[z // nc] = pr[lax.rem(z, share)]

    small(3).wait()
    small(4).wait()
    small(5).wait()

    @pl.loop(0, steps)
    def _(step):
        spread = pl.ds(pl.multiple_of(step * width, width), width)
        sums = jnp.dot(count[...].astype(BF16), table_ref[:, spread], preferred_element_type=F32)
        gate[:, spread] = 1.0 + sums[0:1, :] / acts

    @pl.loop(0, share)
    def _(i):
        @pl.when(i * nc + z // share != z)
        def _():
            got(prr.at[i], p_r.at[i])

    sums = prr[0].astype(F32)
    for t in range(1, share):
        sums = sums + prr[t].astype(F32)
    for j in range(near):
        fin[j] = sums[j * own : (j + 1) * own, :]

    @pl.loop(1, near)
    def _(i):
        j = near_peer(i)
        send(fin.at[j], finr.at[me], f_s.at[j], f_r.at[me], near_id(j))

    finr[me] = fin[me]

    @pl.loop(1, near)
    def _(i):
        j = near_peer(i)
        got(finr.at[j], f_r.at[j])

    even = (lax.broadcasted_iota(jnp.int32, (own, cols), 0) & 1) == 0
    for j in range(near):
        part = slice(j * cols, (j + 1) * cols)
        gates = jnp.where(even, gate[:, part], 1.0 + null_ref[:, part])
        out_ref[:, part] = (res_ref[:, part].astype(F32) + gates * finr[j]).astype(BF16)

    gone(mlp, ml_s)
    gone(wn, wn_s)

    @pl.loop(1, nx)
    def _(i):
        gone(joint, mx_s.at[lax.rem(x + i, nx)])

    @pl.loop(1, near)
    def _(i):
        j = near_peer(i)
        gone(wbuf.at[0], w_s.at[0, j])
        gone(wbuf.at[0], w_s.at[1, j])
        gone(fin.at[0], f_s.at[j])

    @pl.loop(0, near)
    def _(j):
        @pl.when((goal != z) | (j != me))
        def _():
            gone(att, at_s.at[j])

    @pl.loop(0, share)
    def _(n):
        @pl.when(parity * share + n != z)
        def _():
            gone(pr.at[0], p_s.at[n])

    @pl.loop(0, nz)
    def _(t):
        gone(ra.at[pl.ds(0, wide)], a_s.at[t])
        gone(rel.at[0], o_s.at[t])
        gone(fin2.at[0], d_s.at[t])
        gone(relout.at[0], r_s.at[t])

    @pl.loop(1, nz)
    def _(i):
        t = far_peer(i)
        gone(zms.at[0], zm_s.at[t])
        gone(xs.at[0], z_s.at[t])


def run(places, slot_of, cached, actions, queries, keys, values, nk, nv, table, w, null, res):
    nz, nx, nc = places
    near = nx * nc
    rows, model_dim = queries.shape
    half = rows // nc
    heads = model_dim // HEAD
    per_step = 4 if heads % 4 == 0 else 1
    _, frames, tokens, _ = keys.shape
    own = nk.shape[0]
    vocab = table.shape[0]
    wide = model_dim // nz
    blk = wide // nx
    cols = model_dim // near
    wrows = w.shape[0]
    share = nz // nc
    picked = slot_of.shape[0] // nc * frames * tokens + PIECE
    smem = pl.BlockSpec(memory_space=pltpu.SMEM)
    vmem = pl.BlockSpec(memory_space=pltpu.VMEM)
    away = pl.BlockSpec(memory_space=pl.ANY)
    dma = lambda *n: pltpu.SemaphoreType.DMA(n)
    f32 = lambda *n: pltpu.VMEM(n, F32)
    bf16 = lambda *n: pltpu.VMEM(n, BF16)
    large = (queries, nk, nv, table, w, null, res)
    scratch = [pltpu.VMEM(value.shape, value.dtype) for value in large]
    scratch += [bf16(*keys.shape), bf16(*keys.shape)]
    scratch += [dma(3, keys.shape[0]), dma(6)]
    scratch += [
        f32(nc, picked, half), f32(8, vocab), f32(1, model_dim),
        bf16(model_dim, half), f32(model_dim, half), f32(2, 2, heads, half),
        f32(2, heads, half), f32(2, heads, half), f32(2, heads, half),
        f32(nx, 2, heads, half), f32(nx, heads, half),
        bf16(model_dim, half), bf16(model_dim, half),
        *[bf16(nz, blk, half) for _ in range(6)],
        f32(nz, 8, half), f32(nz, 8, half), f32(nz, 8, half), f32(blk, half),
        bf16(wrows, model_dim), bf16(nc, wrows, half), bf16(near, nc, wrows, half),
        bf16(2 * near, wrows, cols),
        bf16(share, half // share, cols), bf16(share, half // share, cols),
        f32(near, own, cols), f32(near, own, cols),
    ]
    scratch += [pltpu.SemaphoreType.DMA, pltpu.SemaphoreType.DMA]
    for size in (nx, nz, nz, nz, nz, nz, nz):
        scratch += [dma(size), dma(size)]
    scratch += [pltpu.SemaphoreType.DMA, pltpu.SemaphoreType.DMA]
    scratch += [dma(near), dma(near), dma(2, near), dma(2, near)]
    scratch += [dma(share), dma(share), dma(near), dma(near)]
    return pl.pallas_call(
        functools.partial(kernel, places, per_step, min(4, nz)),
        in_specs=[smem] * 3 + [away] * 9,
        out_specs=vmem,
        out_shape=jax.ShapeDtypeStruct(res.shape, BF16),
        scratch_shapes=scratch,
        compiler_params=pltpu.CompilerParams(
            collective_id=0, has_side_effects=True, vmem_limit_bytes=67_043_328
        ),
        name="rollout",
    )(slot_of, cached, actions, queries, keys, values, nk, nv, table, w, null, res)


def solution(mesh):
    places = (16, 4, 2)
    split = Mesh(mesh.devices.reshape(mesh.shape["groups"], *places), GROUPS_CTX)

    def on_device(
        queries, new_keys, new_values, cache_keys, cache_values, slot_of, cached, actions,
        action_table, null_gate, residual, out_weight,
    ):
        return run(
            places, slot_of, cached, actions, queries, cache_keys, cache_values, new_keys,
            new_values, action_table, out_weight, null_gate[None, :], residual,
        )

    in_specs = (
        P("groups", None),
        P(GROUPS_CTX, None),
        P(GROUPS_CTX, None),
        P("groups", CTX, None, None),
        P("groups", CTX, None, None),
        P("groups"),
        P("groups"),
        P("groups", None),
        P(),
        P(),
        P(GROUPS_CTX, None),
        P(CTX, None),
    )
    return jax.shard_map(
        on_device, mesh=split, in_specs=in_specs, out_specs=P(GROUPS_CTX, None), check_vma=False
    )
```

```python
import functools
import math

import jax
import jax.numpy as jnp
from jax import lax
from jax.experimental import pallas as pl
from jax.experimental.pallas import tpu as pltpu
from jax.sharding import Mesh
from jax.sharding import PartitionSpec as P

HEAD = 128
PIECE = 16
CTX = ("z", "x", "core")
GROUPS_CTX = ("groups", "z", "x", "core")
MESH = pl.DeviceIdType.MESH
MASKED = -1e30
F32 = jnp.float32
BF16 = jnp.bfloat16
LAST = (((1,), (1,)), ((), ()))
FIRST = (((0,), (0,)), ((), ()))


def kernel(places, per_step, lag, *refs):
    (
        slot_ref, cached_ref, act_ref, q_in, k_in, v_in, nk_in, nv_in, table_in,
        w_in, null_in, res_in, out_ref,
        q_ref, nk_ref, nv_ref, table_ref, w_ref, null_ref, res_ref, k_a, v_a, k_b, v_b, in_s, small_s,
        bias, count, gate, away, home, ml, mlp, scale, joint, mlx, ratio,
        ra, d, rel, relout, fin1, fin2, xs, zr, zms, zmr, fz, acc,
        wn, att, attg, wbuf, pr, prr, fin, finr,
        ml_s, ml_r, mx_s, mx_r, a_s, a_r, o_s, o_r, d_s, d_r, r_s, r_r, z_s, z_r, zm_s, zm_r,
        wn_s, wn_r, at_s, at_r, w_s, w_r, p_s, p_r, f_s, f_r,
    ) = refs
    nz, nx, nc = places
    near = nx * nc
    z, x, c = (lax.axis_index(name) for name in CTX)
    me = x * nc + c
    other = 1 - c
    _, frames, tokens, _ = k_in.shape
    sessions, acts = act_ref.shape
    rows = q_ref.shape[0]
    half = rows // nc
    session_rows = rows // sessions
    mine = sessions // nc
    slot_keys = frames * tokens
    keys = mine * slot_keys
    own = nk_ref.shape[0]
    model_dim = w_ref.shape[1]
    heads = model_dim // HEAD
    wide = model_dim // nz
    blk = wide // nx
    pieces = blk // PIECE
    per_head = HEAD // PIECE
    cols = model_dim // near
    wrows = w_ref.shape[0]
    pos = (z * nx + x) * nc + c
    parity = lax.rem(z, 2)
    twin = z + 1 - 2 * parity
    share = nz // nc
    width = per_step * HEAD
    steps = heads // per_step
    early = k_a.shape[3] // width
    spans = ((0, early, k_a, v_a), (early, steps, k_b, v_b))
    barrier = pltpu.get_barrier_semaphore()

    def near_id(j):
        return {"x": j // nc, "core": lax.rem(j, nc)}

    def twin_id(j):
        return {"z": twin, "x": j // nc, "core": lax.rem(j, nc)}

    def near_peer(i):
        return lax.rem(me + i, near)

    def far_peer(i):
        return lax.rem(z + i, nz)

    def send(src, dst, ssem, rsem, where):
        pltpu.make_async_remote_copy(
            src_ref=src, dst_ref=dst, send_sem=ssem, recv_sem=rsem,
            device_id=where, device_id_type=MESH,
        ).start()

    def half_copy(ref, sem):
        return pltpu.make_async_remote_copy(
            src_ref=ref, dst_ref=ref, send_sem=sem, recv_sem=sem,
            device_id={"core": other}, device_id_type=MESH,
        )

    def got(ref, sem):
        half_copy(ref, sem).wait_recv()

    def gone(ref, sem):
        half_copy(ref, sem).wait_send()

    def greet(where):
        pl.semaphore_signal(barrier, inc=1, device_id=where, device_id_type=MESH)

    smalls = (
        (nk_in, nk_ref), (nv_in, nv_ref), (w_in, w_ref), (table_in, table_ref),
        (null_in, null_ref), (res_in, res_ref),
    )

    def small(n):
        return pltpu.make_async_copy(*smalls[n], small_s.at[n])

    def load(which):
        begin, end, k_to, v_to = spans[which]
        part = slice(begin * width, end * width)
        return [
            pltpu.make_async_copy(k_in.at[:, :, :, part], k_to, in_s.at[0, which]),
            pltpu.make_async_copy(q_in.at[:, part], q_ref.at[:, part], in_s.at[1, which]),
            pltpu.make_async_copy(v_in.at[:, :, :, part], v_to, in_s.at[2, which]),
        ]

    small(0).start()
    small(1).start()
    for copy in load(0):
        copy.start()

    @pl.loop(1, nz)
    def _(i):
        greet({"z": far_peer(i)})

    @pl.loop(1, near)
    def _(i):
        greet(twin_id(near_peer(i)))
        greet(near_id(near_peer(i)))

    key = lax.broadcasted_iota(jnp.int32, (keys, half), 0)
    row = lax.broadcasted_iota(jnp.int32, (keys, half), 1)
    few_key = lax.broadcasted_iota(jnp.int32, (PIECE, half), 0)
    few_row = lax.broadcasted_iota(jnp.int32, (PIECE, half), 1)
    first = pos * own
    session = first // session_rows
    for part in range(nc):
        live = jnp.zeros((keys, half), jnp.int32)
        for s in range(mine):
            alive = cached_ref[part * mine + s] - pos * frames
            alive = jnp.clip(alive, 0, frames) * tokens
            here = (row >= s * session_rows) & (row < (s + 1) * session_rows)
            here = here & (key >= s * slot_keys) & (key < s * slot_keys + alive)
            live = jnp.where(here, 1, live)
        bias[part, 0:keys, :] = jnp.where(live == 1, 0.0, MASKED)
        low = session * session_rows - part * half
        good = (few_row >= low) & (few_row < low + session_rows) & (few_key < own)
        good = good & (((few_row + part * half - first - few_key) & 1) == 0)
        bias[part, keys : keys + PIECE, :] = jnp.where(good, 0.0, MASKED)
    vocab = table_ref.shape[0]
    lane = lax.broadcasted_iota(jnp.int32, (8, vocab), 1)
    sums = jnp.zeros((8, vocab), F32)
    for a in range(acts):
        sums = sums + jnp.where(lane == act_ref[session, a], 1.0, 0.0)
    count[...] = sums

    spot = lax.broadcasted_iota(jnp.int32, (PIECE, HEAD), 0)
    factor = math.log2(math.e) / math.sqrt(HEAD)

    def few(ref, part):
        values = jnp.zeros((PIECE, HEAD), F32)
        for j in range(own):
            values = jnp.where(spot == j, ref[j : j + 1, part].astype(F32), values)
        return values.astype(BF16)

    def taken(ref, extra, part, which):
        parts = []
        for s in range(mine):
            slot = slot_ref[which * mine + s]
            parts.append(ref[slot, :, :, part].reshape(slot_keys, HEAD))
        return jnp.concatenate(parts + [extra], 0)

    small(0).wait()
    small(1).wait()

    def attend(step, begin, k_ref, v_ref):
        work = []
        for i in range(per_step):
            head = step * per_step + i
            part = pl.ds(pl.multiple_of(head * HEAD, HEAD), HEAD)
            into = pl.ds(pl.multiple_of((head - begin * per_step) * HEAD, HEAD), HEAD)
            few_keys = few(nk_ref, part)
            for which in (other, c):
                q = q_ref[pl.ds(pl.multiple_of(which * half, half), half), part]
                k = taken(k_ref, few_keys, into, which)
                s = lax.dot_general(k, q, LAST, preferred_element_type=F32)
                work.append((head, part, into, which, s))
        ready = []
        for head, part, into, which, s in work:
            s = s * factor + bias[which]
            top = jnp.max(s, 0, keepdims=True)
            p = jnp.exp2(s - top)
            total = jnp.sum(p, 0, keepdims=True)
            first = 0 if which is other else 1
            ml[first, 0, pl.ds(head, 1), :] = top
            ml[first, 1, pl.ds(head, 1), :] = total
            ready.append((part, into, which, p.astype(BF16)))
        for part, into, which, p in ready:
            v = taken(v_ref, few(nv_ref, part), into, which)
            numer = lax.dot_general(v, p, FIRST, preferred_element_type=F32)
            if which is other:
                away[part, :] = numer.astype(BF16)
            else:
                home[part, :] = numer

    def pass_on(begin, end):
        @pl.loop(begin * width // wide, end * width // wide)
        def _(t):
            part = pl.ds(pl.multiple_of(t * wide, PIECE), wide)
            send(away.at[part], ra.at[part], a_s, a_r.at[t], {"core": other})

    for copy in load(0):
        copy.wait()
    for copy in load(1):
        copy.start()

    @pl.loop(0, early)
    def _(step):
        attend(step, 0, k_a, v_a)

    pl.semaphore_wait(barrier, nz + 2 * near - 3)
    pass_on(0, early)
    for copy in load(1):
        copy.wait()
    for n in range(2, len(smalls)):
        small(n).start()

    @pl.loop(early, steps)
    def _(step):
        attend(step, early, k_b, v_b)


    def turn(k):
        odd = lax.rem(k, 2)
        ahead = nz // 2 + odd * ((k + 1) // 2) - (1 - odd) * (k // 2)
        return lax.rem(z + ahead, nz)

    def ways(t):
        back = lax.rem(t, 2)
        ahead = lax.rem(x + 1 + (nx - 2) * back, nx)
        behind = lax.rem(x + nx - 1 - (nx - 2) * back, nx)
        return ahead, behind

    opposite = lax.rem(x + nx // 2, nx)

    def rows_of(t, xx):
        return pl.ds(pl.multiple_of(t * wide + xx * blk, PIECE), blk)

    def merge(k):
        t = turn(k)
        got(ra.at[pl.ds(pl.multiple_of(t * wide, PIECE), wide)], a_r.at[t])
        for i in range(wide // PIECE):
            g = t * (wide // PIECE) + i
            h = g // per_head
            r = pl.ds(pl.multiple_of(g * PIECE, PIECE), PIECE)
            here = home[r, :] * scale[0, pl.ds(h, 1), :]
            there = ra[r, :].astype(F32) * scale[1, pl.ds(h, 1), :]
            d[r, :] = (here + there).astype(BF16)
        ahead, behind = ways(t)
        send(d.at[rows_of(t, opposite)], rel.at[t], o_s, o_r.at[t], {"x": ahead})
        send(d.at[rows_of(t, behind)], fin2.at[t], d_s, d_r.at[t], {"x": behind})

    def scaled(t, xx, n):
        g = t * (wide // PIECE) + xx * pieces + n
        h = g // per_head
        r = pl.ds(pl.multiple_of(g * PIECE, PIECE), PIECE)
        return h, d[r, :].astype(F32) * ratio[x, pl.ds(h, 1), :]

    def relay(k):
        t = turn(k)
        ahead, behind = ways(t)
        got(rel.at[t], o_r.at[t])
        for n in range(pieces):
            h, value = scaled(t, ahead, n)
            r = slice(n * PIECE, (n + 1) * PIECE)
            value = value + rel[t, r, :].astype(F32) * ratio[behind, pl.ds(h, 1), :]
            relout[t, r, :] = value.astype(BF16)
        send(relout.at[t], fin1.at[t], r_s, r_r.at[t], {"x": ahead})

    def settle(k):
        t = turn(k)
        ahead, _ = ways(t)
        got(fin1.at[t], r_r.at[t])
        got(fin2.at[t], d_r.at[t])
        for n in range(pieces):
            h, value = scaled(t, x, n)
            r = slice(n * PIECE, (n + 1) * PIECE)
            value = value + fin2[t, r, :].astype(F32) * ratio[ahead, pl.ds(h, 1), :]
            xs[t, r, :] = (value + fin1[t, r, :].astype(F32)).astype(BF16)

        @pl.when(k < nz - 1)
        def _():
            send(xs.at[t], zr.at[z], z_s, z_r.at[z], {"z": t})

    def wpart(j):
        return pl.ds(pl.multiple_of(j * cols, cols), cols)

    def wplace(zz, j):
        return zz * near + j

    send(ml.at[0], mlp, ml_s, ml_r, {"core": other})
    pass_on(early, steps)
    small(2).wait()
    send(w_ref, wn, wn_s, wn_r, {"z": twin})

    got(mlp, ml_r)
    top = jnp.maximum(ml[1, 0], mlp[0])
    here, there = jnp.exp2(ml[1, 0] - top), jnp.exp2(mlp[0] - top)
    scale[0] = here
    scale[1] = there
    joint[0] = top
    joint[1] = ml[1, 1] * here + mlp[1] * there

    @pl.loop(1, nx)
    def _(i):
        xx = lax.rem(x + i, nx)
        send(joint, mlx.at[x], mx_s, mx_r, {"x": xx})

    mlx[x] = joint[...]

    @pl.loop(0, lag)
    def _(k):
        merge(k)

    got(mlx.at[pl.ds(0, nx - 1)], mx_r)

    top = mlx[0, 0]
    for xx in range(1, nx):
        top = jnp.maximum(top, mlx[xx, 0])
    total = jnp.zeros_like(top)
    for xx in range(nx):
        part = jnp.exp2(mlx[xx, 0] - top)
        ratio[xx] = part
        total = total + mlx[xx, 1] * part
    scale2 = mlp
    scale2[0] = top
    scale2[1] = total

    @pl.loop(0, nz)
    def _(t):
        low = (t * (wide // PIECE) + x * pieces) // per_head
        high = jnp.minimum(low + 1, heads - 1)
        zms[t, 0:1, :] = scale2[0, pl.ds(low, 1), :]
        zms[t, 1:2, :] = scale2[0, pl.ds(high, 1), :]
        zms[t, 2:3, :] = scale2[1, pl.ds(low, 1), :]
        zms[t, 3:4, :] = scale2[1, pl.ds(high, 1), :]
        zms[t, 4:8, :] = jnp.zeros((4, half), F32)

    @pl.loop(1, nz)
    def _(i):
        t = far_peer(i)
        send(zms.at[t], zmr.at[z], zm_s, zm_r, {"z": t})

    @pl.loop(lag, nz + 2 * lag)
    def _(k):
        @pl.when(k < nz)
        def _():
            merge(k)

        @pl.when(k < nz + lag)
        def _():
            relay(k - lag)

        @pl.when(k >= 2 * lag)
        def _():
            settle(k - 2 * lag)

    got(wn, wn_r)

    @pl.loop(1, near)
    def _(i):
        j = near_peer(i)
        send(
            w_ref.at[:, wpart(j)], wbuf.at[wplace(parity, me)],
            w_s, w_r, near_id(j),
        )
        send(
            wn.at[:, wpart(j)], wbuf.at[wplace(1 - parity, me)],
            w_s, w_r, near_id(j),
        )

    wbuf[wplace(parity, me)] = w_ref[:, wpart(me)]
    wbuf[wplace(1 - parity, me)] = wn[:, wpart(me)]
    zr[z] = xs[z]
    zmr[z] = zms[z]

    got(zmr.at[pl.ds(0, nz - 1)], zm_r)

    top = zmr[0, 0:2, :]
    for t in range(1, nz):
        top = jnp.maximum(top, zmr[t, 0:2, :])
    total = jnp.zeros_like(top)
    for t in range(nz):
        total = total + zmr[t, 2:4, :] * jnp.exp2(zmr[t, 0:2, :] - top)
    for t in range(nz):
        fz[t, 0:2, :] = jnp.exp2(zmr[t, 0:2, :] - top) / total

    first = z * (wide // PIECE) + x * pieces
    low = first // per_head
    acc[...] = jnp.zeros_like(acc)

    @pl.loop(0, nz)
    def _(i):
        t = far_peer(i)

        @pl.when(i > 0)
        def _():
            got(zr.at[t], z_r.at[t])

        for n in range(pieces):
            r = slice(n * PIECE, (n + 1) * PIECE)
            which = (first + n) // per_head - low
            acc[r, :] = acc[r, :] + zr[t, r, :].astype(F32) * fz[t, pl.ds(which, 1), :]

    for n in range(nc):
        att[n] = acc[n * wrows : (n + 1) * wrows, :].astype(BF16)

    goal = z - parity + c
    spot_of = parity * nx + x

    @pl.loop(0, near)
    def _(i):
        j = near_peer(i)

        @pl.when((goal != z) | (j != me))
        def _():
            send(
                att, attg.at[spot_of], at_s, at_r,
                {"z": goal, "x": j // nc, "core": lax.rem(j, nc)},
            )

    @pl.when(goal == z)
    def _():
        attg[spot_of] = att[...]

    got(wbuf.at[pl.ds(0, 2 * near - 2)], w_r)

    @pl.when(goal == z)
    def _():
        got(attg.at[pl.ds(0, near - 1)], at_r)

    @pl.when(goal != z)
    def _():
        got(attg, at_r)

    product = None
    for i in range(near):
        for n in range(nc):
            term = lax.dot_general(
                attg[i, n], wbuf[i * nc + n], FIRST, preferred_element_type=F32
            )
            product = term if product is None else product + term
    pr[...] = product.astype(BF16).reshape(share, -1, cols)

    def ahead_of(i):
        odd = lax.rem(i, 2)
        skew = odd * ((i + 1) // 2) + (1 - odd) * (share - i // 2)
        near_half = jnp.where(z // share == parity, share // 2, 0)
        return lax.rem(z + near_half + skew, share)

    @pl.loop(0, share)
    def _(i):
        n = ahead_of(i)
        t = parity * share + n

        @pl.when(t != z)
        def _():
            send(pr.at[n], prr.at[z // nc], p_s, p_r, {"z": t})

    @pl.when(z // share == parity)
    def _():
        prr[z // nc] = pr[lax.rem(z, share)]

    small(3).wait()
    small(4).wait()
    small(5).wait()

    @pl.loop(0, steps)
    def _(step):
        spread = pl.ds(pl.multiple_of(step * width, width), width)
        sums = jnp.dot(count[...].astype(BF16), table_ref[:, spread], preferred_element_type=F32)
        gate[:, spread] = 1.0 + sums[0:1, :] / acts

    @pl.when(z // share == parity)
    def _():
        if share > 1:
            got(prr.at[pl.ds(0, share - 1)], p_r)

    @pl.when(z // share != parity)
    def _():
        got(prr, p_r)

    sums = prr[0].astype(F32)
    for t in range(1, share):
        sums = sums + prr[t].astype(F32)
    for j in range(near):
        fin[j] = sums[j * own : (j + 1) * own, :]

    @pl.loop(1, near)
    def _(i):
        j = near_peer(i)
        send(fin.at[j], finr.at[me], f_s, f_r, near_id(j))

    finr[me] = fin[me]

    got(finr.at[pl.ds(0, near - 1)], f_r)

    even = (lax.broadcasted_iota(jnp.int32, (own, cols), 0) & 1) == 0
    for j in range(near):
        part = slice(j * cols, (j + 1) * cols)
        gates = jnp.where(even, gate[:, part], 1.0 + null_ref[:, part])
        out_ref[:, part] = (res_ref[:, part].astype(F32) + gates * finr[j]).astype(BF16)

    gone(mlp, ml_s)
    gone(wn, wn_s)

    gone(mlx.at[pl.ds(0, nx - 1)], mx_s)
    gone(wbuf.at[pl.ds(0, 2 * near - 2)], w_s)
    gone(fin.at[pl.ds(0, near - 1)], f_s)
    gone(ra, a_s)
    gone(rel, o_s)
    gone(fin2, d_s)
    gone(relout, r_s)
    gone(zms.at[pl.ds(0, nz - 1)], zm_s)
    gone(xs.at[pl.ds(0, nz - 1)], z_s)

    @pl.when(goal == z)
    def _():
        gone(attg.at[pl.ds(0, near - 1)], at_s)

    @pl.when(goal != z)
    def _():
        gone(attg, at_s)

    @pl.when(z // share == parity)
    def _():
        if share > 1:
            gone(pr.at[pl.ds(0, share - 1)], p_s)

    @pl.when(z // share != parity)
    def _():
        gone(pr, p_s)


def run(places, slot_of, cached, actions, queries, keys, values, nk, nv, table, w, null, res):
    nz, nx, nc = places
    near = nx * nc
    rows, model_dim = queries.shape
    half = rows // nc
    heads = model_dim // HEAD
    per_step = 4 if heads % 4 == 0 else 1
    _, frames, tokens, _ = keys.shape
    own = nk.shape[0]
    vocab = table.shape[0]
    wide = model_dim // nz
    blk = wide // nx
    cols = model_dim // near
    wrows = w.shape[0]
    share = nz // nc
    picked = slot_of.shape[0] // nc * frames * tokens + PIECE
    smem = pl.BlockSpec(memory_space=pltpu.SMEM)
    vmem = pl.BlockSpec(memory_space=pltpu.VMEM)
    away = pl.BlockSpec(memory_space=pl.ANY)
    dma = lambda *n: pltpu.SemaphoreType.DMA(n)
    f32 = lambda *n: pltpu.VMEM(n, F32)
    bf16 = lambda *n: pltpu.VMEM(n, BF16)
    large = (queries, nk, nv, table, w, null, res)
    scratch = [pltpu.VMEM(value.shape, value.dtype) for value in large]
    early = nz // 2 * wide
    for size in (early, early, model_dim - early, model_dim - early):
        scratch.append(bf16(*keys.shape[:3], size))
    scratch += [dma(3, 2), dma(6)]
    scratch += [
        f32(nc, picked, half), f32(8, vocab), f32(1, model_dim),
        bf16(model_dim, half), f32(model_dim, half), f32(2, 2, heads, half),
        f32(2, heads, half), f32(2, heads, half), f32(2, heads, half),
        f32(nx, 2, heads, half), f32(nx, heads, half),
        bf16(model_dim, half), bf16(model_dim, half),
        *[bf16(nz, blk, half) for _ in range(6)],
        f32(nz, 8, half), f32(nz, 8, half), f32(nz, 8, half), f32(blk, half),
        bf16(wrows, model_dim), bf16(nc, wrows, half), bf16(near, nc, wrows, half),
        bf16(2 * near, wrows, cols),
        bf16(share, half // share, cols), bf16(share, half // share, cols),
        f32(near, own, cols), f32(near, own, cols),
    ]
    one = pltpu.SemaphoreType.DMA
    scratch += [one] * 4
    scratch += [one, dma(nz)] * 5
    scratch += [one] * 12
    return pl.pallas_call(
        functools.partial(kernel, places, per_step, min(4, nz)),
        in_specs=[smem] * 3 + [away] * 9,
        out_specs=vmem,
        out_shape=jax.ShapeDtypeStruct(res.shape, BF16),
        scratch_shapes=scratch,
        compiler_params=pltpu.CompilerParams(
            collective_id=0, has_side_effects=True, vmem_limit_bytes=67_043_328
        ),
        name="rollout",
    )(slot_of, cached, actions, queries, keys, values, nk, nv, table, w, null, res)


def solution(mesh):
    places = (16, 4, 2)
    split = Mesh(mesh.devices.reshape(mesh.shape["groups"], *places), GROUPS_CTX)

    def on_device(
        queries, new_keys, new_values, cache_keys, cache_values, slot_of, cached, actions,
        action_table, null_gate, residual, out_weight,
    ):
        return run(
            places, slot_of, cached, actions, queries, cache_keys, cache_values, new_keys,
            new_values, action_table, out_weight, null_gate[None, :], residual,
        )

    in_specs = (
        P("groups", None),
        P(GROUPS_CTX, None),
        P(GROUPS_CTX, None),
        P("groups", CTX, None, None),
        P("groups", CTX, None, None),
        P("groups"),
        P("groups"),
        P("groups", None),
        P(),
        P(),
        P(GROUPS_CTX, None),
        P(CTX, None),
    )
    return jax.shard_map(
        on_device, mesh=split, in_specs=in_specs, out_specs=P(GROUPS_CTX, None), check_vma=False
    )
```

```python
import functools
import math

import jax
import jax.numpy as jnp
from jax import lax
from jax.experimental import pallas as pl
from jax.experimental.pallas import tpu as pltpu
from jax.sharding import Mesh
from jax.sharding import PartitionSpec as P

HEAD = 128
PIECE = 16
CTX = ("z", "x", "core")
GROUPS_CTX = ("groups", "z", "x", "core")
MESH = pl.DeviceIdType.MESH
MASKED = -1e30
F32 = jnp.float32
BF16 = jnp.bfloat16
LAST = (((1,), (1,)), ((), ()))
FIRST = (((0,), (0,)), ((), ()))


def kernel(places, per_step, lag, *refs):
    (
        slot_ref, cached_ref, act_ref, q_in, k_in, v_in, nk_in, nv_in, table_in,
        w_in, null_in, res_in, out_ref,
        q_ref, nk_ref, nv_ref, table_ref, w_ref, null_ref, res_ref, k_a, v_a, k_b, v_b, in_s, small_s,
        bias, count, gate, away, home, ml, mlp, scale, joint, mlx, ratio,
        ra, d, rel, relout, fin1, fin2, xs, zr, zms, zmr, fz, acc,
        wn, att, attg, wbuf, pr, prr, fin, finr,
        ml_s, ml_r, mx_s, mx_r, a_s, a_r, o_s, o_r, d_s, d_r, r_s, r_r, z_s, z_r, zm_s, zm_r,
        wn_s, wn_r, at_s, at_r, w_s, w_r, p_s, p_r, f_s, f_r,
    ) = refs
    nz, nx, nc = places
    near = nx * nc
    z, x, c = (lax.axis_index(name) for name in CTX)
    me = x * nc + c
    other = 1 - c
    _, frames, tokens, _ = k_in.shape
    sessions, acts = act_ref.shape
    rows = q_ref.shape[0]
    half = rows // nc
    session_rows = rows // sessions
    mine = sessions // nc
    slot_keys = frames * tokens
    keys = mine * slot_keys
    own = nk_ref.shape[0]
    model_dim = w_ref.shape[1]
    heads = model_dim // HEAD
    wide = model_dim // nz
    blk = wide // nx
    pieces = blk // PIECE
    per_head = HEAD // PIECE
    cols = model_dim // near
    wrows = w_ref.shape[0]
    pos = (z * nx + x) * nc + c
    parity = lax.rem(z, 2)
    twin = z + 1 - 2 * parity
    share = nz // nc
    width = per_step * HEAD
    steps = heads // per_step
    early = k_a.shape[3] // width
    spans = ((0, early, k_a, v_a), (early, steps, k_b, v_b))
    barrier = pltpu.get_barrier_semaphore()

    def near_id(j):
        return {"x": j // nc, "core": lax.rem(j, nc)}

    def twin_id(j):
        return {"z": twin, "x": j // nc, "core": lax.rem(j, nc)}

    def near_peer(i):
        return lax.rem(me + i, near)

    def far_peer(i):
        return lax.rem(z + i, nz)

    def send(src, dst, ssem, rsem, where):
        pltpu.make_async_remote_copy(
            src_ref=src, dst_ref=dst, send_sem=ssem, recv_sem=rsem,
            device_id=where, device_id_type=MESH,
        ).start()

    def half_copy(ref, sem):
        return pltpu.make_async_remote_copy(
            src_ref=ref, dst_ref=ref, send_sem=sem, recv_sem=sem,
            device_id={"core": other}, device_id_type=MESH,
        )

    def got(ref, sem):
        half_copy(ref, sem).wait_recv()

    def gone(ref, sem):
        half_copy(ref, sem).wait_send()

    def greet(where):
        pl.semaphore_signal(barrier, inc=1, device_id=where, device_id_type=MESH)

    smalls = (
        (nk_in, nk_ref), (nv_in, nv_ref), (w_in, w_ref), (table_in, table_ref),
        (null_in, null_ref), (res_in, res_ref),
    )

    def small(n):
        return pltpu.make_async_copy(*smalls[n], small_s.at[n])

    def load(which):
        begin, end, k_to, v_to = spans[which]
        part = slice(begin * width, end * width)
        return [
            pltpu.make_async_copy(k_in.at[:, :, :, part], k_to, in_s.at[0, which]),
            pltpu.make_async_copy(q_in.at[:, part], q_ref.at[:, part], in_s.at[1, which]),
            pltpu.make_async_copy(v_in.at[:, :, :, part], v_to, in_s.at[2, which]),
        ]

    def wpart(j):
        return pl.ds(pl.multiple_of(j * cols, cols), cols)

    def wplace(zz, j):
        return zz * near + j

    small(0).start()
    small(1).start()
    for copy in load(0):
        copy.start()
    small(2).start()

    @pl.loop(1, nz)
    def _(i):
        greet({"z": far_peer(i)})

    @pl.loop(1, near)
    def _(i):
        greet(twin_id(near_peer(i)))
        greet(near_id(near_peer(i)))

    key = lax.broadcasted_iota(jnp.int32, (keys, half), 0)
    row = lax.broadcasted_iota(jnp.int32, (keys, half), 1)
    few_key = lax.broadcasted_iota(jnp.int32, (PIECE, half), 0)
    few_row = lax.broadcasted_iota(jnp.int32, (PIECE, half), 1)
    first = pos * own
    session = first // session_rows
    for part in range(nc):
        live = jnp.zeros((keys, half), jnp.int32)
        for s in range(mine):
            alive = cached_ref[part * mine + s] - pos * frames
            alive = jnp.clip(alive, 0, frames) * tokens
            here = (row >= s * session_rows) & (row < (s + 1) * session_rows)
            here = here & (key >= s * slot_keys) & (key < s * slot_keys + alive)
            live = jnp.where(here, 1, live)
        bias[part, 0:keys, :] = jnp.where(live == 1, 0.0, MASKED)
        low = session * session_rows - part * half
        good = (few_row >= low) & (few_row < low + session_rows) & (few_key < own)
        good = good & (((few_row + part * half - first - few_key) & 1) == 0)
        bias[part, keys : keys + PIECE, :] = jnp.where(good, 0.0, MASKED)
    vocab = table_ref.shape[0]
    lane = lax.broadcasted_iota(jnp.int32, (8, vocab), 1)
    sums = jnp.zeros((8, vocab), F32)
    for a in range(acts):
        sums = sums + jnp.where(lane == act_ref[session, a], 1.0, 0.0)
    count[...] = sums

    spot = lax.broadcasted_iota(jnp.int32, (PIECE, HEAD), 0)
    factor = math.log2(math.e) / math.sqrt(HEAD)

    def few(ref, part):
        values = jnp.zeros((PIECE, HEAD), F32)
        for j in range(own):
            values = jnp.where(spot == j, ref[j : j + 1, part].astype(F32), values)
        return values.astype(BF16)

    def taken(ref, extra, part, which):
        parts = []
        for s in range(mine):
            slot = slot_ref[which * mine + s]
            parts.append(ref[slot, :, :, part].reshape(slot_keys, HEAD))
        return jnp.concatenate(parts + [extra], 0)

    small(0).wait()
    small(1).wait()

    def attend(step, begin, k_ref, v_ref):
        work = []
        for i in range(per_step):
            head = step * per_step + i
            part = pl.ds(pl.multiple_of(head * HEAD, HEAD), HEAD)
            into = pl.ds(pl.multiple_of((head - begin * per_step) * HEAD, HEAD), HEAD)
            few_keys = few(nk_ref, part)
            for which in (other, c):
                q = q_ref[pl.ds(pl.multiple_of(which * half, half), half), part]
                k = taken(k_ref, few_keys, into, which)
                s = lax.dot_general(k, q, LAST, preferred_element_type=F32)
                work.append((head, part, into, which, s))
        ready = []
        for head, part, into, which, s in work:
            s = s * factor + bias[which]
            top = jnp.max(s, 0, keepdims=True)
            p = jnp.exp2(s - top)
            total = jnp.sum(p, 0, keepdims=True)
            first = 0 if which is other else 1
            ml[first, 0, pl.ds(head, 1), :] = top
            ml[first, 1, pl.ds(head, 1), :] = total
            ready.append((part, into, which, p.astype(BF16)))
        for part, into, which, p in ready:
            v = taken(v_ref, few(nv_ref, part), into, which)
            numer = lax.dot_general(v, p, FIRST, preferred_element_type=F32)
            if which is other:
                away[part, :] = numer.astype(BF16)
            else:
                home[part, :] = numer

    def pass_on(begin, end):
        @pl.loop(begin * width // wide, end * width // wide)
        def _(t):
            part = pl.ds(pl.multiple_of(t * wide, PIECE), wide)
            send(away.at[part], ra.at[part], a_s, a_r.at[t], {"core": other})

    for copy in load(0):
        copy.wait()
    for copy in load(1):
        copy.start()

    @pl.loop(0, early)
    def _(step):
        attend(step, 0, k_a, v_a)

    pl.semaphore_wait(barrier, nz + 2 * near - 3)
    pass_on(0, early)
    small(2).wait()
    send(w_ref, wn, wn_s, wn_r, {"z": twin})

    @pl.loop(1, near)
    def _(i):
        j = near_peer(i)
        send(w_ref.at[:, wpart(j)], wbuf.at[wplace(parity, me)], w_s, w_r, near_id(j))

    for copy in load(1):
        copy.wait()
    for n in range(3, len(smalls)):
        small(n).start()

    @pl.loop(early, steps)
    def _(step):
        attend(step, early, k_b, v_b)


    def turn(k):
        odd = lax.rem(k, 2)
        ahead = nz // 2 + odd * ((k + 1) // 2) - (1 - odd) * (k // 2)
        return lax.rem(z + ahead, nz)

    def ways(t):
        back = lax.rem(t, 2)
        ahead = lax.rem(x + 1 + (nx - 2) * back, nx)
        behind = lax.rem(x + nx - 1 - (nx - 2) * back, nx)
        return ahead, behind

    opposite = lax.rem(x + nx // 2, nx)

    def rows_of(t, xx):
        return pl.ds(pl.multiple_of(t * wide + xx * blk, PIECE), blk)

    def merge(k):
        t = turn(k)
        got(ra.at[pl.ds(pl.multiple_of(t * wide, PIECE), wide)], a_r.at[t])
        for i in range(wide // PIECE):
            g = t * (wide // PIECE) + i
            h = g // per_head
            r = pl.ds(pl.multiple_of(g * PIECE, PIECE), PIECE)
            here = home[r, :] * scale[0, pl.ds(h, 1), :]
            there = ra[r, :].astype(F32) * scale[1, pl.ds(h, 1), :]
            d[r, :] = (here + there).astype(BF16)
        ahead, behind = ways(t)
        send(d.at[rows_of(t, opposite)], rel.at[t], o_s, o_r.at[t], {"x": ahead})
        send(d.at[rows_of(t, behind)], fin2.at[t], d_s, d_r.at[t], {"x": behind})

    def scaled(t, xx, n):
        g = t * (wide // PIECE) + xx * pieces + n
        h = g // per_head
        r = pl.ds(pl.multiple_of(g * PIECE, PIECE), PIECE)
        return h, d[r, :].astype(F32) * ratio[x, pl.ds(h, 1), :]

    def relay(k):
        t = turn(k)
        ahead, behind = ways(t)
        got(rel.at[t], o_r.at[t])
        for n in range(pieces):
            h, value = scaled(t, ahead, n)
            r = slice(n * PIECE, (n + 1) * PIECE)
            value = value + rel[t, r, :].astype(F32) * ratio[behind, pl.ds(h, 1), :]
            relout[t, r, :] = value.astype(BF16)
        send(relout.at[t], fin1.at[t], r_s, r_r.at[t], {"x": ahead})

    def settle(k):
        t = turn(k)
        ahead, _ = ways(t)
        got(fin1.at[t], r_r.at[t])
        got(fin2.at[t], d_r.at[t])
        for n in range(pieces):
            h, value = scaled(t, x, n)
            r = slice(n * PIECE, (n + 1) * PIECE)
            value = value + fin2[t, r, :].astype(F32) * ratio[ahead, pl.ds(h, 1), :]
            xs[t, r, :] = (value + fin1[t, r, :].astype(F32)).astype(BF16)

        @pl.when(k < nz - 1)
        def _():
            send(xs.at[t], zr.at[z], z_s, z_r.at[z], {"z": t})

    send(ml.at[0], mlp, ml_s, ml_r, {"core": other})
    pass_on(early, steps)

    got(mlp, ml_r)
    top = jnp.maximum(ml[1, 0], mlp[0])
    here, there = jnp.exp2(ml[1, 0] - top), jnp.exp2(mlp[0] - top)
    scale[0] = here
    scale[1] = there
    joint[0] = top
    joint[1] = ml[1, 1] * here + mlp[1] * there

    @pl.loop(1, nx)
    def _(i):
        xx = lax.rem(x + i, nx)
        send(joint, mlx.at[x], mx_s, mx_r, {"x": xx})

    mlx[x] = joint[...]

    @pl.loop(0, lag)
    def _(k):
        merge(k)

    got(mlx.at[pl.ds(0, nx - 1)], mx_r)

    top = mlx[0, 0]
    for xx in range(1, nx):
        top = jnp.maximum(top, mlx[xx, 0])
    total = jnp.zeros_like(top)
    for xx in range(nx):
        part = jnp.exp2(mlx[xx, 0] - top)
        ratio[xx] = part
        total = total + mlx[xx, 1] * part
    scale2 = mlp
    scale2[0] = top
    scale2[1] = total

    @pl.loop(0, nz)
    def _(t):
        low = (t * (wide // PIECE) + x * pieces) // per_head
        high = jnp.minimum(low + 1, heads - 1)
        zms[t, 0:1, :] = scale2[0, pl.ds(low, 1), :]
        zms[t, 1:2, :] = scale2[0, pl.ds(high, 1), :]
        zms[t, 2:3, :] = scale2[1, pl.ds(low, 1), :]
        zms[t, 3:4, :] = scale2[1, pl.ds(high, 1), :]
        zms[t, 4:8, :] = jnp.zeros((4, half), F32)

    @pl.loop(1, nz)
    def _(i):
        t = far_peer(i)
        send(zms.at[t], zmr.at[z], zm_s, zm_r, {"z": t})

    @pl.loop(lag, nz + 2 * lag)
    def _(k):
        @pl.when(k < nz)
        def _():
            merge(k)

        @pl.when(k < nz + lag)
        def _():
            relay(k - lag)

        @pl.when(k >= 2 * lag)
        def _():
            settle(k - 2 * lag)

    got(wn, wn_r)

    @pl.loop(1, near)
    def _(i):
        j = near_peer(i)
        send(
            wn.at[:, wpart(j)], wbuf.at[wplace(1 - parity, me)],
            w_s, w_r, near_id(j),
        )

    wbuf[wplace(parity, me)] = w_ref[:, wpart(me)]
    wbuf[wplace(1 - parity, me)] = wn[:, wpart(me)]
    zr[z] = xs[z]
    zmr[z] = zms[z]

    got(zmr.at[pl.ds(0, nz - 1)], zm_r)

    top = zmr[0, 0:2, :]
    for t in range(1, nz):
        top = jnp.maximum(top, zmr[t, 0:2, :])
    total = jnp.zeros_like(top)
    for t in range(nz):
        total = total + zmr[t, 2:4, :] * jnp.exp2(zmr[t, 0:2, :] - top)
    for t in range(nz):
        fz[t, 0:2, :] = jnp.exp2(zmr[t, 0:2, :] - top) / total

    first = z * (wide // PIECE) + x * pieces
    low = first // per_head
    acc[...] = jnp.zeros_like(acc)

    @pl.loop(0, nz)
    def _(i):
        t = far_peer(i)

        @pl.when(i > 0)
        def _():
            got(zr.at[t], z_r.at[t])

        for n in range(pieces):
            r = slice(n * PIECE, (n + 1) * PIECE)
            which = (first + n) // per_head - low
            acc[r, :] = acc[r, :] + zr[t, r, :].astype(F32) * fz[t, pl.ds(which, 1), :]

    for n in range(nc):
        att[n] = acc[n * wrows : (n + 1) * wrows, :].astype(BF16)

    goal = z - parity + c
    spot_of = parity * nx + x

    @pl.loop(0, near)
    def _(i):
        j = near_peer(i)

        @pl.when((goal != z) | (j != me))
        def _():
            send(
                att, attg.at[spot_of], at_s, at_r,
                {"z": goal, "x": j // nc, "core": lax.rem(j, nc)},
            )

    @pl.when(goal == z)
    def _():
        attg[spot_of] = att[...]

    got(wbuf.at[pl.ds(0, 2 * near - 2)], w_r)

    @pl.when(goal == z)
    def _():
        got(attg.at[pl.ds(0, near - 1)], at_r)

    @pl.when(goal != z)
    def _():
        got(attg, at_r)

    product = None
    for i in range(near):
        for n in range(nc):
            term = lax.dot_general(
                attg[i, n], wbuf[i * nc + n], FIRST, preferred_element_type=F32
            )
            product = term if product is None else product + term
    pr[...] = product.astype(BF16).reshape(share, -1, cols)

    def ahead_of(i):
        odd = lax.rem(i, 2)
        skew = odd * ((i + 1) // 2) + (1 - odd) * (share - i // 2)
        near_half = jnp.where(z // share == parity, share // 2, 0)
        return lax.rem(z + near_half + skew, share)

    @pl.loop(0, share)
    def _(i):
        n = ahead_of(i)
        t = parity * share + n

        @pl.when(t != z)
        def _():
            send(pr.at[n], prr.at[z // nc], p_s, p_r, {"z": t})

    @pl.when(z // share == parity)
    def _():
        prr[z // nc] = pr[lax.rem(z, share)]

    small(3).wait()
    small(4).wait()
    small(5).wait()

    @pl.loop(0, steps)
    def _(step):
        spread = pl.ds(pl.multiple_of(step * width, width), width)
        sums = jnp.dot(count[...].astype(BF16), table_ref[:, spread], preferred_element_type=F32)
        gate[:, spread] = 1.0 + sums[0:1, :] / acts

    @pl.when(z // share == parity)
    def _():
        if share > 1:
            got(prr.at[pl.ds(0, share - 1)], p_r)

    @pl.when(z // share != parity)
    def _():
        got(prr, p_r)

    sums = prr[0].astype(F32)
    for t in range(1, share):
        sums = sums + prr[t].astype(F32)
    for j in range(near):
        fin[j] = sums[j * own : (j + 1) * own, :]

    @pl.loop(1, near)
    def _(i):
        j = near_peer(i)
        send(fin.at[j], finr.at[me], f_s, f_r, near_id(j))

    finr[me] = fin[me]

    got(finr.at[pl.ds(0, near - 1)], f_r)

    even = (lax.broadcasted_iota(jnp.int32, (own, cols), 0) & 1) == 0
    for j in range(near):
        part = slice(j * cols, (j + 1) * cols)
        gates = jnp.where(even, gate[:, part], 1.0 + null_ref[:, part])
        out_ref[:, part] = (res_ref[:, part].astype(F32) + gates * finr[j]).astype(BF16)

    gone(mlp, ml_s)
    gone(wn, wn_s)

    gone(mlx.at[pl.ds(0, nx - 1)], mx_s)
    gone(wbuf.at[pl.ds(0, 2 * near - 2)], w_s)
    gone(fin.at[pl.ds(0, near - 1)], f_s)
    gone(ra, a_s)
    gone(rel, o_s)
    gone(fin2, d_s)
    gone(relout, r_s)
    gone(zms.at[pl.ds(0, nz - 1)], zm_s)
    gone(xs.at[pl.ds(0, nz - 1)], z_s)

    @pl.when(goal == z)
    def _():
        gone(attg.at[pl.ds(0, near - 1)], at_s)

    @pl.when(goal != z)
    def _():
        gone(attg, at_s)

    @pl.when(z // share == parity)
    def _():
        if share > 1:
            gone(pr.at[pl.ds(0, share - 1)], p_s)

    @pl.when(z // share != parity)
    def _():
        gone(pr, p_s)


def run(places, slot_of, cached, actions, queries, keys, values, nk, nv, table, w, null, res):
    nz, nx, nc = places
    near = nx * nc
    rows, model_dim = queries.shape
    half = rows // nc
    heads = model_dim // HEAD
    per_step = 4 if heads % 4 == 0 else 1
    _, frames, tokens, _ = keys.shape
    own = nk.shape[0]
    vocab = table.shape[0]
    wide = model_dim // nz
    blk = wide // nx
    cols = model_dim // near
    wrows = w.shape[0]
    share = nz // nc
    picked = slot_of.shape[0] // nc * frames * tokens + PIECE
    smem = pl.BlockSpec(memory_space=pltpu.SMEM)
    vmem = pl.BlockSpec(memory_space=pltpu.VMEM)
    away = pl.BlockSpec(memory_space=pl.ANY)
    dma = lambda *n: pltpu.SemaphoreType.DMA(n)
    f32 = lambda *n: pltpu.VMEM(n, F32)
    bf16 = lambda *n: pltpu.VMEM(n, BF16)
    large = (queries, nk, nv, table, w, null, res)
    scratch = [pltpu.VMEM(value.shape, value.dtype) for value in large]
    early = nz // 2 * wide
    for size in (early, early, model_dim - early, model_dim - early):
        scratch.append(bf16(*keys.shape[:3], size))
    scratch += [dma(3, 2), dma(6)]
    scratch += [
        f32(nc, picked, half), f32(8, vocab), f32(1, model_dim),
        bf16(model_dim, half), f32(model_dim, half), f32(2, 2, heads, half),
        f32(2, heads, half), f32(2, heads, half), f32(2, heads, half),
        f32(nx, 2, heads, half), f32(nx, heads, half),
        bf16(model_dim, half), bf16(model_dim, half),
        *[bf16(nz, blk, half) for _ in range(6)],
        f32(nz, 8, half), f32(nz, 8, half), f32(nz, 8, half), f32(blk, half),
        bf16(wrows, model_dim), bf16(nc, wrows, half), bf16(near, nc, wrows, half),
        bf16(2 * near, wrows, cols),
        bf16(share, half // share, cols), bf16(share, half // share, cols),
        f32(near, own, cols), f32(near, own, cols),
    ]
    one = pltpu.SemaphoreType.DMA
    scratch += [one] * 4
    scratch += [one, dma(nz)] * 5
    scratch += [one] * 12
    return pl.pallas_call(
        functools.partial(kernel, places, per_step, min(4, nz)),
        in_specs=[smem] * 3 + [away] * 9,
        out_specs=vmem,
        out_shape=jax.ShapeDtypeStruct(res.shape, BF16),
        scratch_shapes=scratch,
        compiler_params=pltpu.CompilerParams(
            collective_id=0, has_side_effects=True, vmem_limit_bytes=67_043_328
        ),
        name="rollout",
    )(slot_of, cached, actions, queries, keys, values, nk, nv, table, w, null, res)


def solution(mesh):
    places = (16, 4, 2)
    split = Mesh(mesh.devices.reshape(mesh.shape["groups"], *places), GROUPS_CTX)

    def on_device(
        queries, new_keys, new_values, cache_keys, cache_values, slot_of, cached, actions,
        action_table, null_gate, residual, out_weight,
    ):
        return run(
            places, slot_of, cached, actions, queries, cache_keys, cache_values, new_keys,
            new_values, action_table, out_weight, null_gate[None, :], residual,
        )

    in_specs = (
        P("groups", None),
        P(GROUPS_CTX, None),
        P(GROUPS_CTX, None),
        P("groups", CTX, None, None),
        P("groups", CTX, None, None),
        P("groups"),
        P("groups"),
        P("groups", None),
        P(),
        P(),
        P(GROUPS_CTX, None),
        P(CTX, None),
    )
    return jax.shard_map(
        on_device, mesh=split, in_specs=in_specs, out_specs=P(GROUPS_CTX, None), check_vma=False
    )
```

```python
import functools
import math

import jax
import jax.numpy as jnp
from jax import lax
from jax.experimental import pallas as pl
from jax.experimental.pallas import tpu as pltpu
from jax.sharding import Mesh
from jax.sharding import PartitionSpec as P

HEAD = 128
PIECE = 16
CTX = ("z", "x", "core")
GROUPS_CTX = ("groups", "z", "x", "core")
MESH = pl.DeviceIdType.MESH
MASKED = -1e30
F32 = jnp.float32
BF16 = jnp.bfloat16
LAST = (((1,), (1,)), ((), ()))
FIRST = (((0,), (0,)), ((), ()))


def kernel(places, per_step, lag, *refs):
    (
        slot_ref, cached_ref, act_ref, q_in, k_in, v_in, nk_in, nv_in, table_in,
        w_in, null_in, res_in, out_ref,
        q_ref, nk_ref, nv_ref, table_ref, w_ref, null_ref, res_ref, k_a, v_a, k_b, v_b, in_s, small_s,
        bias, count, gate, away, home, ml, mlp, scale, joint, mlx, ratio,
        ra, d, rel, relout, fin1, fin2, xs, zr, zms, zmr, fz, acc,
        wn, att, attg, wbuf, pr, prr, fin, finr,
        ml_s, ml_r, mx_s, mx_r, a_s, a_r, o_s, o_r, d_s, d_r, r_s, r_r, z_s, z_r, zm_s, zm_r,
        wn_s, wn_r, at_s, at_r, w_s, w_r, p_s, p_r, f_s, f_r,
    ) = refs
    nz, nx, nc = places
    near = nx * nc
    z, x, c = (lax.axis_index(name) for name in CTX)
    me = x * nc + c
    other = 1 - c
    _, frames, tokens, _ = k_in.shape
    sessions, acts = act_ref.shape
    rows = q_ref.shape[0]
    half = rows // nc
    session_rows = rows // sessions
    mine = sessions // nc
    slot_keys = frames * tokens
    keys = mine * slot_keys
    own = nk_ref.shape[0]
    model_dim = w_ref.shape[1]
    heads = model_dim // HEAD
    wide = model_dim // nz
    blk = wide // nx
    pieces = blk // PIECE
    per_head = HEAD // PIECE
    cols = model_dim // near
    wrows = w_ref.shape[0]
    pos = (z * nx + x) * nc + c
    parity = lax.rem(z, 2)
    twin = z + 1 - 2 * parity
    share = nz // nc
    width = per_step * HEAD
    steps = heads // per_step
    early = k_a.shape[3] // width
    spans = ((0, early, k_a, v_a), (early, steps, k_b, v_b))
    barrier = pltpu.get_barrier_semaphore()

    def near_id(j):
        return {"x": j // nc, "core": lax.rem(j, nc)}

    def twin_id(j):
        return {"z": twin, "x": j // nc, "core": lax.rem(j, nc)}

    def near_peer(i):
        return lax.rem(me + i, near)

    def far_peer(i):
        return lax.rem(z + i, nz)

    def send(src, dst, ssem, rsem, where):
        pltpu.make_async_remote_copy(
            src_ref=src, dst_ref=dst, send_sem=ssem, recv_sem=rsem,
            device_id=where, device_id_type=MESH,
        ).start()

    def half_copy(ref, sem):
        return pltpu.make_async_remote_copy(
            src_ref=ref, dst_ref=ref, send_sem=sem, recv_sem=sem,
            device_id={"core": other}, device_id_type=MESH,
        )

    def got(ref, sem):
        half_copy(ref, sem).wait_recv()

    def gone(ref, sem):
        half_copy(ref, sem).wait_send()

    def greet(where):
        pl.semaphore_signal(barrier, inc=1, device_id=where, device_id_type=MESH)

    smalls = (
        (nk_in, nk_ref), (nv_in, nv_ref), (w_in, w_ref), (table_in, table_ref),
        (null_in, null_ref), (res_in, res_ref),
    )

    def small(n):
        return pltpu.make_async_copy(*smalls[n], small_s.at[n])

    def load(which):
        begin, end, k_to, v_to = spans[which]
        part = slice(begin * width, end * width)
        return [
            pltpu.make_async_copy(k_in.at[:, :, :, part], k_to, in_s.at[0, which]),
            pltpu.make_async_copy(q_in.at[:, part], q_ref.at[:, part], in_s.at[1, which]),
            pltpu.make_async_copy(v_in.at[:, :, :, part], v_to, in_s.at[2, which]),
        ]

    def wpart(j):
        return pl.ds(pl.multiple_of(j * cols, cols), cols)

    def wplace(zz, j):
        return zz * near + j

    small(0).start()
    small(1).start()
    for copy in load(0):
        copy.start()
    small(2).start()

    @pl.loop(1, nz)
    def _(i):
        greet({"z": far_peer(i)})

    @pl.loop(1, near)
    def _(i):
        greet(twin_id(near_peer(i)))
        greet(near_id(near_peer(i)))

    key = lax.broadcasted_iota(jnp.int32, (keys, half), 0)
    row = lax.broadcasted_iota(jnp.int32, (keys, half), 1)
    few_key = lax.broadcasted_iota(jnp.int32, (PIECE, half), 0)
    few_row = lax.broadcasted_iota(jnp.int32, (PIECE, half), 1)
    first = pos * own
    session = first // session_rows
    for part in range(nc):
        live = jnp.zeros((keys, half), jnp.int32)
        for s in range(mine):
            alive = cached_ref[part * mine + s] - pos * frames
            alive = jnp.clip(alive, 0, frames) * tokens
            here = (row >= s * session_rows) & (row < (s + 1) * session_rows)
            here = here & (key >= s * slot_keys) & (key < s * slot_keys + alive)
            live = jnp.where(here, 1, live)
        bias[part, 0:keys, :] = jnp.where(live == 1, 0.0, MASKED)
        low = session * session_rows - part * half
        good = (few_row >= low) & (few_row < low + session_rows) & (few_key < own)
        good = good & (((few_row + part * half - first - few_key) & 1) == 0)
        bias[part, keys : keys + PIECE, :] = jnp.where(good, 0.0, MASKED)
    vocab = table_ref.shape[0]
    lane = lax.broadcasted_iota(jnp.int32, (8, vocab), 1)
    sums = jnp.zeros((8, vocab), F32)
    for a in range(acts):
        sums = sums + jnp.where(lane == act_ref[session, a], 1.0, 0.0)
    count[...] = sums

    spot = lax.broadcasted_iota(jnp.int32, (PIECE, HEAD), 0)
    factor = math.log2(math.e) / math.sqrt(HEAD)

    def few(ref, part):
        values = jnp.zeros((PIECE, HEAD), F32)
        for j in range(own):
            values = jnp.where(spot == j, ref[j : j + 1, part].astype(F32), values)
        return values.astype(BF16)

    def taken(ref, extra, part, which):
        parts = []
        for s in range(mine):
            slot = slot_ref[which * mine + s]
            parts.append(ref[slot, :, :, part].reshape(slot_keys, HEAD))
        return jnp.concatenate(parts + [extra], 0)

    small(0).wait()
    small(1).wait()

    def attend(step, begin, k_ref, v_ref):
        work = []
        for i in range(per_step):
            head = step * per_step + i
            part = pl.ds(pl.multiple_of(head * HEAD, HEAD), HEAD)
            into = pl.ds(pl.multiple_of((head - begin * per_step) * HEAD, HEAD), HEAD)
            few_keys = few(nk_ref, part)
            for which in (other, c):
                q = q_ref[pl.ds(pl.multiple_of(which * half, half), half), part]
                k = taken(k_ref, few_keys, into, which)
                s = lax.dot_general(k, q, LAST, preferred_element_type=F32)
                work.append((head, part, into, which, s))
        ready = []
        for head, part, into, which, s in work:
            s = s * factor + bias[which]
            top = jnp.max(s, 0, keepdims=True)
            p = jnp.exp2(s - top)
            total = jnp.sum(p, 0, keepdims=True)
            first = 0 if which is other else 1
            ml[first, 0, pl.ds(head, 1), :] = top
            ml[first, 1, pl.ds(head, 1), :] = total
            ready.append((part, into, which, p.astype(BF16)))
        for part, into, which, p in ready:
            v = taken(v_ref, few(nv_ref, part), into, which)
            numer = lax.dot_general(v, p, FIRST, preferred_element_type=F32)
            if which is other:
                away[part, :] = numer.astype(BF16)
            else:
                home[part, :] = numer

    def pass_on(begin, end):
        @pl.loop(begin * width // wide, end * width // wide)
        def _(t):
            part = pl.ds(pl.multiple_of(t * wide, PIECE), wide)
            send(away.at[part], ra.at[part], a_s, a_r.at[t], {"core": other})

    for copy in load(0):
        copy.wait()
    for copy in load(1):
        copy.start()

    @pl.loop(0, early)
    def _(step):
        attend(step, 0, k_a, v_a)

    pl.semaphore_wait(barrier, nz + 2 * near - 3)
    pass_on(0, early)
    small(2).wait()
    send(w_ref, wn, wn_s, wn_r, {"z": twin})

    @pl.loop(1, near)
    def _(i):
        j = near_peer(i)
        send(w_ref.at[:, wpart(j)], wbuf.at[wplace(parity, me)], w_s, w_r, near_id(j))

    for copy in load(1):
        copy.wait()
    for n in range(3, len(smalls)):
        small(n).start()

    @pl.loop(early, steps)
    def _(step):
        attend(step, early, k_b, v_b)


    def turn(k):
        odd = lax.rem(k, 2)
        ahead = nz // 2 + odd * ((k + 1) // 2) - (1 - odd) * (k // 2)
        return lax.rem(z + ahead, nz)

    def ways(t):
        back = lax.rem(t, 2)
        ahead = lax.rem(x + 1 + (nx - 2) * back, nx)
        behind = lax.rem(x + nx - 1 - (nx - 2) * back, nx)
        return ahead, behind

    opposite = lax.rem(x + nx // 2, nx)

    def rows_of(t, xx):
        return pl.ds(pl.multiple_of(t * wide + xx * blk, PIECE), blk)

    def merge(k):
        t = turn(k)
        got(ra.at[pl.ds(pl.multiple_of(t * wide, PIECE), wide)], a_r.at[t])
        for i in range(wide // PIECE):
            g = t * (wide // PIECE) + i
            h = g // per_head
            r = pl.ds(pl.multiple_of(g * PIECE, PIECE), PIECE)
            here = home[r, :] * scale[0, pl.ds(h, 1), :]
            there = ra[r, :].astype(F32) * scale[1, pl.ds(h, 1), :]
            d[r, :] = (here + there).astype(BF16)
        ahead, behind = ways(t)
        send(d.at[rows_of(t, opposite)], rel.at[t], o_s, o_r.at[t], {"x": ahead})
        send(d.at[rows_of(t, behind)], fin2.at[t], d_s, d_r.at[t], {"x": behind})

    def scaled(t, xx, n):
        g = t * (wide // PIECE) + xx * pieces + n
        h = g // per_head
        r = pl.ds(pl.multiple_of(g * PIECE, PIECE), PIECE)
        return h, d[r, :].astype(F32) * ratio[x, pl.ds(h, 1), :]

    def relay(k):
        t = turn(k)
        ahead, behind = ways(t)
        got(rel.at[t], o_r.at[t])
        for n in range(pieces):
            h, value = scaled(t, ahead, n)
            r = slice(n * PIECE, (n + 1) * PIECE)
            value = value + rel[t, r, :].astype(F32) * ratio[behind, pl.ds(h, 1), :]
            relout[t, r, :] = value.astype(BF16)
        send(relout.at[t], fin1.at[t], r_s, r_r.at[t], {"x": ahead})

    def settle(k):
        t = turn(k)
        ahead, _ = ways(t)
        got(fin1.at[t], r_r.at[t])
        got(fin2.at[t], d_r.at[t])
        for n in range(pieces):
            h, value = scaled(t, x, n)
            r = slice(n * PIECE, (n + 1) * PIECE)
            value = value + fin2[t, r, :].astype(F32) * ratio[ahead, pl.ds(h, 1), :]
            xs[t, r, :] = (value + fin1[t, r, :].astype(F32)).astype(BF16)

        @pl.when(k < nz - 1)
        def _():
            send(xs.at[t], zr.at[z], z_s, z_r.at[z], {"z": t})

    send(ml.at[0], mlp, ml_s, ml_r, {"core": other})
    pass_on(early, steps)

    got(mlp, ml_r)
    top = jnp.maximum(ml[1, 0], mlp[0])
    here, there = jnp.exp2(ml[1, 0] - top), jnp.exp2(mlp[0] - top)
    scale[0] = here
    scale[1] = there
    joint[0] = top
    joint[1] = ml[1, 1] * here + mlp[1] * there

    @pl.loop(1, nx)
    def _(i):
        xx = lax.rem(x + i, nx)
        send(joint, mlx.at[x], mx_s, mx_r, {"x": xx})

    mlx[x] = joint[...]

    @pl.loop(0, lag)
    def _(k):
        merge(k)

    got(mlx.at[pl.ds(0, nx - 1)], mx_r)

    top = mlx[0, 0]
    for xx in range(1, nx):
        top = jnp.maximum(top, mlx[xx, 0])
    total = jnp.zeros_like(top)
    for xx in range(nx):
        part = jnp.exp2(mlx[xx, 0] - top)
        ratio[xx] = part
        total = total + mlx[xx, 1] * part
    scale2 = mlp
    scale2[0] = top
    scale2[1] = total

    @pl.loop(0, nz)
    def _(t):
        low = (t * (wide // PIECE) + x * pieces) // per_head
        high = jnp.minimum(low + 1, heads - 1)
        zms[t, 0:1, :] = scale2[0, pl.ds(low, 1), :]
        zms[t, 1:2, :] = scale2[0, pl.ds(high, 1), :]
        zms[t, 2:3, :] = scale2[1, pl.ds(low, 1), :]
        zms[t, 3:4, :] = scale2[1, pl.ds(high, 1), :]

    @pl.loop(1, nz)
    def _(i):
        t = far_peer(i)
        send(zms.at[t], zmr.at[z], zm_s, zm_r, {"z": t})

    def twin_columns():
        got(wn, wn_r)

        @pl.loop(1, near)
        def _(i):
            j = near_peer(i)
            send(
                wn.at[:, wpart(j)], wbuf.at[wplace(1 - parity, me)],
                w_s, w_r, near_id(j),
            )

    @pl.loop(lag, nz + 2 * lag)
    def _(k):
        @pl.when(k < nz)
        def _():
            merge(k)

        @pl.when(k < nz + lag)
        def _():
            relay(k - lag)

        @pl.when(k == nz + lag - 1)
        def _():
            twin_columns()

        @pl.when(k >= 2 * lag)
        def _():
            settle(k - 2 * lag)

    wbuf[wplace(parity, me)] = w_ref[:, wpart(me)]
    wbuf[wplace(1 - parity, me)] = wn[:, wpart(me)]
    zr[z] = xs[z]
    zmr[z] = zms[z]

    got(zmr.at[pl.ds(0, nz - 1)], zm_r)

    top = zmr[0, 0:2, :]
    for t in range(1, nz):
        top = jnp.maximum(top, zmr[t, 0:2, :])
    total = jnp.zeros_like(top)
    for t in range(nz):
        total = total + zmr[t, 2:4, :] * jnp.exp2(zmr[t, 0:2, :] - top)
    for t in range(nz):
        fz[t, 0:2, :] = jnp.exp2(zmr[t, 0:2, :] - top) / total

    first = z * (wide // PIECE) + x * pieces
    low = first // per_head
    acc[...] = jnp.zeros_like(acc)

    @pl.loop(0, nz)
    def _(i):
        t = far_peer(i)

        @pl.when(i > 0)
        def _():
            got(zr.at[t], z_r.at[t])

        for n in range(pieces):
            r = slice(n * PIECE, (n + 1) * PIECE)
            which = (first + n) // per_head - low
            acc[r, :] = acc[r, :] + zr[t, r, :].astype(F32) * fz[t, pl.ds(which, 1), :]

    for n in range(nc):
        att[n] = acc[n * wrows : (n + 1) * wrows, :].astype(BF16)

    goal = z - parity + c
    spot_of = parity * nx + x

    @pl.loop(0, near)
    def _(i):
        j = near_peer(i)

        @pl.when((goal != z) | (j != me))
        def _():
            send(
                att, attg.at[spot_of], at_s, at_r,
                {"z": goal, "x": j // nc, "core": lax.rem(j, nc)},
            )

    @pl.when(goal == z)
    def _():
        attg[spot_of] = att[...]

    got(wbuf.at[pl.ds(0, 2 * near - 2)], w_r)

    @pl.when(goal == z)
    def _():
        got(attg.at[pl.ds(0, near - 1)], at_r)

    @pl.when(goal != z)
    def _():
        got(attg, at_r)

    product = None
    for i in range(near):
        for n in range(nc):
            term = lax.dot_general(
                attg[i, n], wbuf[i * nc + n], FIRST, preferred_element_type=F32
            )
            product = term if product is None else product + term
    pr[...] = product.astype(BF16).reshape(share, -1, cols)

    def ahead_of(i):
        odd = lax.rem(i, 2)
        skew = odd * ((i + 1) // 2) + (1 - odd) * (share - i // 2)
        near_half = jnp.where(z // share == parity, share // 2, 0)
        return lax.rem(z + near_half + skew, share)

    @pl.loop(0, share)
    def _(i):
        n = ahead_of(i)
        t = parity * share + n

        @pl.when(t != z)
        def _():
            send(pr.at[n], prr.at[z // nc], p_s, p_r, {"z": t})

    @pl.when(z // share == parity)
    def _():
        prr[z // nc] = pr[lax.rem(z, share)]

    small(3).wait()
    small(4).wait()
    small(5).wait()

    @pl.loop(0, steps)
    def _(step):
        spread = pl.ds(pl.multiple_of(step * width, width), width)
        sums = jnp.dot(count[...].astype(BF16), table_ref[:, spread], preferred_element_type=F32)
        gate[:, spread] = 1.0 + sums[0:1, :] / acts

    @pl.when(z // share == parity)
    def _():
        if share > 1:
            got(prr.at[pl.ds(0, share - 1)], p_r)

    @pl.when(z // share != parity)
    def _():
        got(prr, p_r)

    sums = prr[0].astype(F32)
    for t in range(1, share):
        sums = sums + prr[t].astype(F32)
    for j in range(near):
        fin[j] = sums[j * own : (j + 1) * own, :]

    @pl.loop(1, near)
    def _(i):
        j = near_peer(i)
        send(fin.at[j], finr.at[me], f_s, f_r, near_id(j))

    finr[me] = fin[me]

    got(finr.at[pl.ds(0, near - 1)], f_r)

    even = (lax.broadcasted_iota(jnp.int32, (own, cols), 0) & 1) == 0
    for j in range(near):
        part = slice(j * cols, (j + 1) * cols)
        gates = jnp.where(even, gate[:, part], 1.0 + null_ref[:, part])
        out_ref[:, part] = (res_ref[:, part].astype(F32) + gates * finr[j]).astype(BF16)

    gone(mlp, ml_s)
    gone(wn, wn_s)

    gone(mlx.at[pl.ds(0, nx - 1)], mx_s)
    gone(wbuf.at[pl.ds(0, 2 * near - 2)], w_s)
    gone(fin.at[pl.ds(0, near - 1)], f_s)
    gone(ra, a_s)
    gone(rel, o_s)
    gone(fin2, d_s)
    gone(relout, r_s)
    gone(zms.at[pl.ds(0, nz - 1)], zm_s)
    gone(xs.at[pl.ds(0, nz - 1)], z_s)

    @pl.when(goal == z)
    def _():
        gone(attg.at[pl.ds(0, near - 1)], at_s)

    @pl.when(goal != z)
    def _():
        gone(attg, at_s)

    @pl.when(z // share == parity)
    def _():
        if share > 1:
            gone(pr.at[pl.ds(0, share - 1)], p_s)

    @pl.when(z // share != parity)
    def _():
        gone(pr, p_s)


def run(places, slot_of, cached, actions, queries, keys, values, nk, nv, table, w, null, res):
    nz, nx, nc = places
    near = nx * nc
    rows, model_dim = queries.shape
    half = rows // nc
    heads = model_dim // HEAD
    per_step = 4 if heads % 4 == 0 else 1
    _, frames, tokens, _ = keys.shape
    own = nk.shape[0]
    vocab = table.shape[0]
    wide = model_dim // nz
    blk = wide // nx
    cols = model_dim // near
    wrows = w.shape[0]
    share = nz // nc
    picked = slot_of.shape[0] // nc * frames * tokens + PIECE
    smem = pl.BlockSpec(memory_space=pltpu.SMEM)
    vmem = pl.BlockSpec(memory_space=pltpu.VMEM)
    away = pl.BlockSpec(memory_space=pl.ANY)
    dma = lambda *n: pltpu.SemaphoreType.DMA(n)
    f32 = lambda *n: pltpu.VMEM(n, F32)
    bf16 = lambda *n: pltpu.VMEM(n, BF16)
    large = (queries, nk, nv, table, w, null, res)
    scratch = [pltpu.VMEM(value.shape, value.dtype) for value in large]
    early = nz // 2 * wide
    for size in (early, early, model_dim - early, model_dim - early):
        scratch.append(bf16(*keys.shape[:3], size))
    scratch += [dma(3, 2), dma(6)]
    scratch += [
        f32(nc, picked, half), f32(8, vocab), f32(1, model_dim),
        bf16(model_dim, half), f32(model_dim, half), f32(2, 2, heads, half),
        f32(2, heads, half), f32(2, heads, half), f32(2, heads, half),
        f32(nx, 2, heads, half), f32(nx, heads, half),
        bf16(model_dim, half), bf16(model_dim, half),
        *[bf16(nz, blk, half) for _ in range(6)],
        f32(nz, 4, half), f32(nz, 4, half), f32(nz, 8, half), f32(blk, half),
        bf16(wrows, model_dim), bf16(nc, wrows, half), bf16(near, nc, wrows, half),
        bf16(2 * near, wrows, cols),
        bf16(share, half // share, cols), bf16(share, half // share, cols),
        f32(near, own, cols), f32(near, own, cols),
    ]
    one = pltpu.SemaphoreType.DMA
    scratch += [one] * 4
    scratch += [one, dma(nz)] * 5
    scratch += [one] * 12
    return pl.pallas_call(
        functools.partial(kernel, places, per_step, min(4, nz)),
        in_specs=[smem] * 3 + [away] * 9,
        out_specs=vmem,
        out_shape=jax.ShapeDtypeStruct(res.shape, BF16),
        scratch_shapes=scratch,
        compiler_params=pltpu.CompilerParams(
            collective_id=0, has_side_effects=True, vmem_limit_bytes=67_043_328
        ),
        name="rollout",
    )(slot_of, cached, actions, queries, keys, values, nk, nv, table, w, null, res)


def solution(mesh):
    places = (16, 4, 2)
    split = Mesh(mesh.devices.reshape(mesh.shape["groups"], *places), GROUPS_CTX)

    def on_device(
        queries, new_keys, new_values, cache_keys, cache_values, slot_of, cached, actions,
        action_table, null_gate, residual, out_weight,
    ):
        return run(
            places, slot_of, cached, actions, queries, cache_keys, cache_values, new_keys,
            new_values, action_table, out_weight, null_gate[None, :], residual,
        )

    in_specs = (
        P("groups", None),
        P(GROUPS_CTX, None),
        P(GROUPS_CTX, None),
        P("groups", CTX, None, None),
        P("groups", CTX, None, None),
        P("groups"),
        P("groups"),
        P("groups", None),
        P(),
        P(),
        P(GROUPS_CTX, None),
        P(CTX, None),
    )
    return jax.shard_map(
        on_device, mesh=split, in_specs=in_specs, out_specs=P(GROUPS_CTX, None), check_vma=False
    )
```

```python
import functools
import math

import jax
import jax.numpy as jnp
from jax import lax
from jax.experimental import pallas as pl
from jax.experimental.pallas import tpu as pltpu
from jax.sharding import Mesh
from jax.sharding import PartitionSpec as P

HEAD = 128
PIECE = 16
CTX = ("z", "x", "core")
GROUPS_CTX = ("groups", "z", "x", "core")
MESH = pl.DeviceIdType.MESH
MASKED = -1e30
F32 = jnp.float32
BF16 = jnp.bfloat16
LAST = (((1,), (1,)), ((), ()))
FIRST = (((0,), (0,)), ((), ()))


def kernel(places, per_step, lag, *refs):
    (
        slot_ref, cached_ref, act_ref, q_in, k_in, v_in, nk_in, nv_in, table_in,
        w_in, null_in, res_in, out_ref,
        q_ref, nk_ref, nv_ref, table_ref, w_ref, null_ref, res_ref, k_a, v_a, k_b, v_b, in_s, small_s,
        bias, count, gate, away, home, ml, mlp, scale, joint, mlx, ratio,
        ra, d, rel, relout, fin1, fin2, xs, zr, zms, zmr, fz, acc,
        wn, att, attg, wbuf, pr, prr, fin, finr,
        ml_s, ml_r, mx_s, mx_r, a_s, a_r, o_s, o_r, d_s, d_r, r_s, r_r, z_s, z_r, zm_s, zm_r,
        wn_s, wn_r, at_s, at_r, w_s, w_r, p_s, p_r, f_s, f_r,
    ) = refs
    nz, nx, nc = places
    near = nx * nc
    z, x, c = (lax.axis_index(name) for name in CTX)
    me = x * nc + c
    other = 1 - c
    _, frames, tokens, _ = k_in.shape
    sessions, acts = act_ref.shape
    rows = q_ref.shape[0]
    half = rows // nc
    session_rows = rows // sessions
    mine = sessions // nc
    slot_keys = frames * tokens
    keys = mine * slot_keys
    own = nk_ref.shape[0]
    model_dim = w_ref.shape[1]
    heads = model_dim // HEAD
    wide = model_dim // nz
    blk = wide // nx
    pieces = blk // PIECE
    per_head = HEAD // PIECE
    cols = model_dim // near
    wrows = w_ref.shape[0]
    pos = (z * nx + x) * nc + c
    parity = lax.rem(z, 2)
    twin = z + 1 - 2 * parity
    share = nz // nc
    width = per_step * HEAD
    steps = heads // per_step
    early = k_a.shape[3] // width
    spans = ((0, early, k_a, v_a), (early, steps, k_b, v_b))
    barrier = pltpu.get_barrier_semaphore()

    def near_id(j):
        return {"x": j // nc, "core": lax.rem(j, nc)}

    def twin_id(j):
        return {"z": twin, "x": j // nc, "core": lax.rem(j, nc)}

    def near_peer(i):
        return lax.rem(me + i, near)

    def far_peer(i):
        return lax.rem(z + i, nz)

    def send(src, dst, ssem, rsem, where):
        pltpu.make_async_remote_copy(
            src_ref=src, dst_ref=dst, send_sem=ssem, recv_sem=rsem,
            device_id=where, device_id_type=MESH,
        ).start()

    def half_copy(ref, sem):
        return pltpu.make_async_remote_copy(
            src_ref=ref, dst_ref=ref, send_sem=sem, recv_sem=sem,
            device_id={"core": other}, device_id_type=MESH,
        )

    def got(ref, sem):
        half_copy(ref, sem).wait_recv()

    def gone(ref, sem):
        half_copy(ref, sem).wait_send()

    def greet(where):
        pl.semaphore_signal(barrier, inc=1, device_id=where, device_id_type=MESH)

    smalls = (
        (nk_in, nk_ref), (nv_in, nv_ref), (w_in, w_ref), (table_in, table_ref),
        (null_in, null_ref), (res_in, res_ref),
    )

    def small(n):
        return pltpu.make_async_copy(*smalls[n], small_s.at[n])

    def load(which):
        begin, end, k_to, v_to = spans[which]
        part = slice(begin * width, end * width)
        return [
            pltpu.make_async_copy(k_in.at[:, :, :, part], k_to, in_s.at[0, which]),
            pltpu.make_async_copy(q_in.at[:, part], q_ref.at[:, part], in_s.at[1, which]),
            pltpu.make_async_copy(v_in.at[:, :, :, part], v_to, in_s.at[2, which]),
        ]

    def wpart(j):
        return pl.ds(pl.multiple_of(j * cols, cols), cols)

    def wplace(zz, j):
        return zz * near + j

    small(0).start()
    small(1).start()
    for copy in load(0):
        copy.start()
    small(2).start()

    @pl.loop(1, nz)
    def _(i):
        greet({"z": far_peer(i)})

    @pl.loop(1, near)
    def _(i):
        greet(twin_id(near_peer(i)))
        greet(near_id(near_peer(i)))

    key = lax.broadcasted_iota(jnp.int32, (keys, half), 0)
    row = lax.broadcasted_iota(jnp.int32, (keys, half), 1)
    few_key = lax.broadcasted_iota(jnp.int32, (PIECE, half), 0)
    few_row = lax.broadcasted_iota(jnp.int32, (PIECE, half), 1)
    first = pos * own
    session = first // session_rows
    for part in range(nc):
        live = jnp.zeros((keys, half), jnp.int32)
        for s in range(mine):
            alive = cached_ref[part * mine + s] - pos * frames
            alive = jnp.clip(alive, 0, frames) * tokens
            here = (row >= s * session_rows) & (row < (s + 1) * session_rows)
            here = here & (key >= s * slot_keys) & (key < s * slot_keys + alive)
            live = jnp.where(here, 1, live)
        bias[part, 0:keys, :] = jnp.where(live == 1, 0.0, MASKED)
        low = session * session_rows - part * half
        good = (few_row >= low) & (few_row < low + session_rows) & (few_key < own)
        good = good & (((few_row + part * half - first - few_key) & 1) == 0)
        bias[part, keys : keys + PIECE, :] = jnp.where(good, 0.0, MASKED)
    vocab = table_ref.shape[0]
    lane = lax.broadcasted_iota(jnp.int32, (8, vocab), 1)
    sums = jnp.zeros((8, vocab), F32)
    for a in range(acts):
        sums = sums + jnp.where(lane == act_ref[session, a], 1.0, 0.0)
    count[...] = sums

    spot = lax.broadcasted_iota(jnp.int32, (PIECE, HEAD), 0)
    factor = math.log2(math.e) / math.sqrt(HEAD)

    def few(ref, part):
        values = jnp.zeros((PIECE, HEAD), F32)
        for j in range(own):
            values = jnp.where(spot == j, ref[j : j + 1, part].astype(F32), values)
        return values.astype(BF16)

    def taken(ref, extra, part, which):
        parts = []
        for s in range(mine):
            slot = slot_ref[which * mine + s]
            parts.append(ref[slot, :, :, part].reshape(slot_keys, HEAD))
        return jnp.concatenate(parts + [extra], 0)

    small(0).wait()
    small(1).wait()

    def attend(step, begin, k_ref, v_ref):
        work = []
        for i in range(per_step):
            head = step * per_step + i
            part = pl.ds(pl.multiple_of(head * HEAD, HEAD), HEAD)
            into = pl.ds(pl.multiple_of((head - begin * per_step) * HEAD, HEAD), HEAD)
            few_keys = few(nk_ref, part)
            for which in (other, c):
                q = q_ref[pl.ds(pl.multiple_of(which * half, half), half), part]
                k = taken(k_ref, few_keys, into, which)
                s = lax.dot_general(k, q, LAST, preferred_element_type=F32)
                work.append((head, part, into, which, s))
        ready = []
        for head, part, into, which, s in work:
            s = s * factor + bias[which]
            top = jnp.max(s, 0, keepdims=True)
            p = jnp.exp2(s - top)
            total = jnp.sum(p, 0, keepdims=True)
            first = 0 if which is other else 1
            ml[first, 0, pl.ds(head, 1), :] = top
            ml[first, 1, pl.ds(head, 1), :] = total
            ready.append((part, into, which, p.astype(BF16)))
        for part, into, which, p in ready:
            v = taken(v_ref, few(nv_ref, part), into, which)
            numer = lax.dot_general(v, p, FIRST, preferred_element_type=F32)
            if which is other:
                away[part, :] = numer.astype(BF16)
            else:
                home[part, :] = numer

    def pass_on(begin, end):
        @pl.loop(begin * width // wide, end * width // wide)
        def _(t):
            part = pl.ds(pl.multiple_of(t * wide, PIECE), wide)
            send(away.at[part], ra.at[part], a_s, a_r.at[t], {"core": other})

    for copy in load(0):
        copy.wait()
    for copy in load(1):
        copy.start()

    @pl.loop(0, early)
    def _(step):
        attend(step, 0, k_a, v_a)

    pl.semaphore_wait(barrier, nz + 2 * near - 3)
    pass_on(0, early)
    small(2).wait()
    send(w_ref, wn, wn_s, wn_r, {"z": twin})

    @pl.loop(1, near)
    def _(i):
        j = near_peer(i)
        send(w_ref.at[:, wpart(j)], wbuf.at[wplace(parity, me)], w_s, w_r, near_id(j))

    for copy in load(1):
        copy.wait()
    for n in range(3, len(smalls)):
        small(n).start()

    @pl.loop(early, steps)
    def _(step):
        attend(step, early, k_b, v_b)


    def turn(k):
        odd = lax.rem(k, 2)
        ahead = nz // 2 + odd * ((k + 1) // 2) - (1 - odd) * (k // 2)
        return lax.rem(z + ahead, nz)

    def ways(t):
        back = lax.rem(t, 2)
        ahead = lax.rem(x + 1 + (nx - 2) * back, nx)
        behind = lax.rem(x + nx - 1 - (nx - 2) * back, nx)
        return ahead, behind

    opposite = lax.rem(x + nx // 2, nx)

    def rows_of(t, xx):
        return pl.ds(pl.multiple_of(t * wide + xx * blk, PIECE), blk)

    def merge(k):
        t = turn(k)
        got(ra.at[pl.ds(pl.multiple_of(t * wide, PIECE), wide)], a_r.at[t])
        for i in range(wide // PIECE):
            g = t * (wide // PIECE) + i
            h = g // per_head
            r = pl.ds(pl.multiple_of(g * PIECE, PIECE), PIECE)
            here = home[r, :] * scale[0, pl.ds(h, 1), :]
            there = ra[r, :].astype(F32) * scale[1, pl.ds(h, 1), :]
            d[r, :] = (here + there).astype(BF16)
        ahead, behind = ways(t)
        send(d.at[rows_of(t, opposite)], rel.at[t], o_s, o_r.at[t], {"x": ahead})
        send(d.at[rows_of(t, behind)], fin2.at[t], d_s, d_r.at[t], {"x": behind})

    def scaled(t, xx, n):
        g = t * (wide // PIECE) + xx * pieces + n
        h = g // per_head
        r = pl.ds(pl.multiple_of(g * PIECE, PIECE), PIECE)
        return h, d[r, :].astype(F32) * ratio[x, pl.ds(h, 1), :]

    def relay(k):
        t = turn(k)
        ahead, behind = ways(t)
        got(rel.at[t], o_r.at[t])
        for n in range(pieces):
            h, value = scaled(t, ahead, n)
            r = slice(n * PIECE, (n + 1) * PIECE)
            value = value + rel[t, r, :].astype(F32) * ratio[behind, pl.ds(h, 1), :]
            relout[t, r, :] = value.astype(BF16)
        send(relout.at[t], fin1.at[t], r_s, r_r.at[t], {"x": ahead})

    def settle(k):
        t = turn(k)
        ahead, _ = ways(t)
        got(fin1.at[t], r_r.at[t])
        got(fin2.at[t], d_r.at[t])
        for n in range(pieces):
            h, value = scaled(t, x, n)
            r = slice(n * PIECE, (n + 1) * PIECE)
            value = value + fin2[t, r, :].astype(F32) * ratio[ahead, pl.ds(h, 1), :]
            xs[t, r, :] = (value + fin1[t, r, :].astype(F32)).astype(BF16)

        @pl.when(k < nz - 1)
        def _():
            send(xs.at[t], zr.at[z], z_s, z_r.at[z], {"z": t})

    send(ml.at[0], mlp, ml_s, ml_r, {"core": other})
    pass_on(early, steps)

    got(mlp, ml_r)
    top = jnp.maximum(ml[1, 0], mlp[0])
    here, there = jnp.exp2(ml[1, 0] - top), jnp.exp2(mlp[0] - top)
    scale[0] = here
    scale[1] = there
    joint[0] = top
    joint[1] = ml[1, 1] * here + mlp[1] * there

    @pl.loop(1, nx)
    def _(i):
        xx = lax.rem(x + i, nx)
        send(joint, mlx.at[x], mx_s, mx_r, {"x": xx})

    mlx[x] = joint[...]

    @pl.loop(0, lag)
    def _(k):
        merge(k)

    got(mlx.at[pl.ds(0, nx - 1)], mx_r)

    top = mlx[0, 0]
    for xx in range(1, nx):
        top = jnp.maximum(top, mlx[xx, 0])
    total = jnp.zeros_like(top)
    for xx in range(nx):
        part = jnp.exp2(mlx[xx, 0] - top)
        ratio[xx] = part
        total = total + mlx[xx, 1] * part
    scale2 = mlp
    scale2[0] = top
    scale2[1] = total

    @pl.loop(0, nz)
    def _(t):
        low = (t * (wide // PIECE) + x * pieces) // per_head
        high = jnp.minimum(low + 1, heads - 1)
        zms[t, 0:1, :] = scale2[0, pl.ds(low, 1), :]
        zms[t, 1:2, :] = scale2[0, pl.ds(high, 1), :]
        zms[t, 2:3, :] = scale2[1, pl.ds(low, 1), :]
        zms[t, 3:4, :] = scale2[1, pl.ds(high, 1), :]

    @pl.loop(1, nz)
    def _(i):
        t = far_peer(i)
        send(zms.at[t], zmr.at[z], zm_s, zm_r, {"z": t})

    def twin_columns():
        got(wn, wn_r)

        @pl.loop(1, near)
        def _(i):
            j = near_peer(i)
            send(
                wn.at[:, wpart(j)], wbuf.at[wplace(1 - parity, me)],
                w_s, w_r, near_id(j),
            )

    @pl.loop(lag, nz + 2 * lag)
    def _(k):
        @pl.when(k < nz)
        def _():
            merge(k)

        @pl.when(k < nz + lag)
        def _():
            relay(k - lag)

        @pl.when(k == nz + lag - 1)
        def _():
            twin_columns()

        @pl.when(k >= 2 * lag)
        def _():
            settle(k - 2 * lag)

    wbuf[wplace(parity, me)] = w_ref[:, wpart(me)]
    wbuf[wplace(1 - parity, me)] = wn[:, wpart(me)]
    zr[z] = xs[z]
    zmr[z] = zms[z]

    got(zmr.at[pl.ds(0, nz - 1)], zm_r)

    top = zmr[0, 0:2, :]
    for t in range(1, nz):
        top = jnp.maximum(top, zmr[t, 0:2, :])
    total = jnp.zeros_like(top)
    for t in range(nz):
        total = total + zmr[t, 2:4, :] * jnp.exp2(zmr[t, 0:2, :] - top)
    for t in range(nz):
        fz[t, 0:2, :] = jnp.exp2(zmr[t, 0:2, :] - top) / total

    first = z * (wide // PIECE) + x * pieces
    low = first // per_head
    acc[...] = jnp.zeros_like(acc)

    @pl.loop(0, nz)
    def _(i):
        t = far_peer(i)

        @pl.when(i > 0)
        def _():
            got(zr.at[t], z_r.at[t])

        for n in range(pieces):
            r = slice(n * PIECE, (n + 1) * PIECE)
            which = (first + n) // per_head - low
            acc[r, :] = acc[r, :] + zr[t, r, :].astype(F32) * fz[t, pl.ds(which, 1), :]

    for n in range(nc):
        att[n] = acc[n * wrows : (n + 1) * wrows, :].astype(BF16)

    goal = z - parity + c
    spot_of = parity * nx + x

    @pl.loop(0, near)
    def _(i):
        j = near_peer(i)

        @pl.when((goal != z) | (j != me))
        def _():
            send(
                att, attg.at[spot_of], at_s, at_r,
                {"z": goal, "x": j // nc, "core": lax.rem(j, nc)},
            )

    @pl.when(goal == z)
    def _():
        attg[spot_of] = att[...]

    got(wbuf.at[pl.ds(0, 2 * near - 2)], w_r)

    @pl.when(goal == z)
    def _():
        got(attg.at[pl.ds(0, near - 1)], at_r)

    @pl.when(goal != z)
    def _():
        got(attg, at_r)

    product = None
    for i in range(near):
        for n in range(nc):
            term = lax.dot_general(
                attg[i, n], wbuf[i * nc + n], FIRST, preferred_element_type=F32
            )
            product = term if product is None else product + term
    pr[...] = product.astype(BF16).reshape(share, -1, cols)

    def ahead_of(i):
        odd = lax.rem(i, 2)
        skew = odd * ((i + 1) // 2) + (1 - odd) * (share - i // 2)
        near_half = jnp.where(z // share == parity, share // 2, 0)
        return lax.rem(z + near_half + skew, share)

    @pl.loop(0, share)
    def _(i):
        n = ahead_of(i)
        t = parity * share + n

        @pl.when(t != z)
        def _():
            send(pr.at[n], prr.at[z // nc], p_s, p_r, {"z": t})

    @pl.when(z // share == parity)
    def _():
        prr[z // nc] = pr[lax.rem(z, share)]

    small(3).wait()
    small(4).wait()
    small(5).wait()

    @pl.loop(0, steps)
    def _(step):
        spread = pl.ds(pl.multiple_of(step * width, width), width)
        sums = jnp.dot(count[...].astype(BF16), table_ref[:, spread], preferred_element_type=F32)
        gate[:, spread] = 1.0 + sums[0:1, :] / acts

    @pl.when(z // share == parity)
    def _():
        if share > 1:
            got(prr.at[pl.ds(0, share - 1)], p_r)

    @pl.when(z // share != parity)
    def _():
        got(prr, p_r)

    sums = prr[0].astype(F32)
    for t in range(1, share):
        sums = sums + prr[t].astype(F32)
    for j in range(near):
        fin[j] = sums[j * own : (j + 1) * own, :]

    @pl.loop(1, near)
    def _(i):
        j = near_peer(i)
        send(fin.at[j], finr.at[me], f_s, f_r, near_id(j))

    finr[me] = fin[me]

    got(finr.at[pl.ds(0, near - 1)], f_r)

    even = (lax.broadcasted_iota(jnp.int32, (own, cols), 0) & 1) == 0
    for j in range(near):
        part = slice(j * cols, (j + 1) * cols)
        gates = jnp.where(even, gate[:, part], 1.0 + null_ref[:, part])
        out_ref[:, part] = (res_ref[:, part].astype(F32) + gates * finr[j]).astype(BF16)

    gone(mlp, ml_s)
    gone(wn, wn_s)

    gone(mlx.at[pl.ds(0, nx - 1)], mx_s)
    gone(wbuf.at[pl.ds(0, 2 * near - 2)], w_s)
    gone(fin.at[pl.ds(0, near - 1)], f_s)
    gone(ra, a_s)
    gone(rel, o_s)
    gone(fin2, d_s)
    gone(relout, r_s)
    gone(zms.at[pl.ds(0, nz - 1)], zm_s)
    gone(xs.at[pl.ds(0, nz - 1)], z_s)

    @pl.when(goal == z)
    def _():
        gone(attg.at[pl.ds(0, near - 1)], at_s)

    @pl.when(goal != z)
    def _():
        gone(attg, at_s)

    @pl.when(z // share == parity)
    def _():
        if share > 1:
            gone(pr.at[pl.ds(0, share - 1)], p_s)

    @pl.when(z // share != parity)
    def _():
        gone(pr, p_s)


def run(places, slot_of, cached, actions, queries, keys, values, nk, nv, table, w, null, res):
    nz, nx, nc = places
    near = nx * nc
    rows, model_dim = queries.shape
    half = rows // nc
    heads = model_dim // HEAD
    per_step = 4 if heads % 4 == 0 else 1
    _, frames, tokens, _ = keys.shape
    own = nk.shape[0]
    vocab = table.shape[0]
    wide = model_dim // nz
    blk = wide // nx
    cols = model_dim // near
    wrows = w.shape[0]
    share = nz // nc
    picked = slot_of.shape[0] // nc * frames * tokens + PIECE
    smem = pl.BlockSpec(memory_space=pltpu.SMEM)
    vmem = pl.BlockSpec(memory_space=pltpu.VMEM)
    away = pl.BlockSpec(memory_space=pl.ANY)
    dma = lambda *n: pltpu.SemaphoreType.DMA(n)
    f32 = lambda *n: pltpu.VMEM(n, F32)
    bf16 = lambda *n: pltpu.VMEM(n, BF16)
    large = (queries, nk, nv, table, w, null, res)
    scratch = [pltpu.VMEM(value.shape, value.dtype) for value in large]
    early = nz // 2 * wide
    for size in (early, early, model_dim - early, model_dim - early):
        scratch.append(bf16(*keys.shape[:3], size))
    scratch += [dma(3, 2), dma(6)]
    scratch += [
        f32(nc, picked, half), f32(8, vocab), f32(1, model_dim),
        bf16(model_dim, half), f32(model_dim, half), f32(2, 2, heads, half),
        f32(2, heads, half), f32(2, heads, half), f32(2, heads, half),
        f32(nx, 2, heads, half), f32(nx, heads, half),
        bf16(model_dim, half), bf16(model_dim, half),
        *[bf16(nz, blk, half) for _ in range(6)],
        f32(nz, 4, half), f32(nz, 4, half), f32(nz, 8, half), f32(blk, half),
        bf16(wrows, model_dim), bf16(nc, wrows, half), bf16(near, nc, wrows, half),
        bf16(2 * near, wrows, cols),
        bf16(share, half // share, cols), bf16(share, half // share, cols),
        f32(near, own, cols), f32(near, own, cols),
    ]
    one = pltpu.SemaphoreType.DMA
    scratch += [one] * 4
    scratch += [one, dma(nz)] * 5
    scratch += [one] * 12
    return pl.pallas_call(
        functools.partial(kernel, places, per_step, min(3, nz)),
        in_specs=[smem] * 3 + [away] * 9,
        out_specs=vmem,
        out_shape=jax.ShapeDtypeStruct(res.shape, BF16),
        scratch_shapes=scratch,
        compiler_params=pltpu.CompilerParams(
            collective_id=0, has_side_effects=True, vmem_limit_bytes=67_043_328
        ),
        name="rollout",
    )(slot_of, cached, actions, queries, keys, values, nk, nv, table, w, null, res)


def solution(mesh):
    places = (16, 4, 2)
    split = Mesh(mesh.devices.reshape(mesh.shape["groups"], *places), GROUPS_CTX)

    def on_device(
        queries, new_keys, new_values, cache_keys, cache_values, slot_of, cached, actions,
        action_table, null_gate, residual, out_weight,
    ):
        return run(
            places, slot_of, cached, actions, queries, cache_keys, cache_values, new_keys,
            new_values, action_table, out_weight, null_gate[None, :], residual,
        )

    in_specs = (
        P("groups", None),
        P(GROUPS_CTX, None),
        P(GROUPS_CTX, None),
        P("groups", CTX, None, None),
        P("groups", CTX, None, None),
        P("groups"),
        P("groups"),
        P("groups", None),
        P(),
        P(),
        P(GROUPS_CTX, None),
        P(CTX, None),
    )
    return jax.shard_map(
        on_device, mesh=split, in_specs=in_specs, out_specs=P(GROUPS_CTX, None), check_vma=False
    )
```
